32 devices in a mesh: band: 4 (over z), ga: 8 (over y, x, core).
Axes of the slice: x: 2, y: 2, z: 4, core: 2. Of those that a mesh axis runs over, the one named last changes fastest.
Arguments:
- coeffs: float32 [2, 4, 18432], P(None, 'band', 'ga'), may hold values from -8 to 8
- cell_map: int32 [18432], P('ga'), may hold values from 0 to 110591, as said below
- potential: float32 [96, 96, 96], P(None, 'ga'), may hold values from -2 to 1
- projectors: float32 [2, 64, 18432], P(None, None, 'ga'), may hold values from -6 to 6
- strengths: float32 [8, 8, 8], replicated, may hold values from -2 to 2
- proj_atom: int32 [64], replicated, may hold values from 0 to 7, as said below
- proj_chan: int32 [64], replicated, may hold values from 0 to 7, as said below
Outputs:
- new_bands: float32 [2, 4, 18432], P(None, 'band', 'ga')
- energy: float32 [4], P('band')
- residual_norm: float32 [4], P('band')
- correlation: float32 [2, 4, 4], P(None, 'band')
- subspace: float32 [2, 4, 4], P(None, 'band')
The draws below stay inside these ranges and needn't reach their ends.
Inputs may be any that keep to these rules, and one draw needn't show every extreme that they name: `cell_map`: in block d (entries d * 2304 to (d + 1) * 2304 - 1) the entries are distinct cells (i * 96 + y) * 96 + z of grid planes x = d + 8 * i. `proj_atom`: each pair of atom and channel belongs to exactly one projector. `proj_chan`: each pair of atom and channel belongs to exactly one projector.
All inputs are finite; a program needn't handle non-finite values.
Results may differ from the reference program's by a relative error of at most 0.0002.
Values sent between devices are 32-bit elements; how exact they have to be, the bound alone decides.
A program may use at most 64 MiB of HBM per device.

```python
import jax
import jax.numpy as jnp
from jax import lax

NG = 96
PW_DEV = 2304
NATOM = 8
NCH = 8
NPROJ = 64
PW_BLOCKS = 8
NPW = 18432
NBANDS = 4


kin_unit = 0.02


def signed_freq_drawn(index_arr):
    return jnp.where(index_arr < NG // 2, index_arr, index_arr - NG)


def sphere_cells(key):
    block_count = NPW // PW_DEV
    planes = NG // block_count
    slab_cells = planes * NG * NG
    cell_ids = jnp.arange(slab_cells, dtype=jnp.int32)
    plane_num = cell_ids // (NG * NG)
    freq_y = signed_freq_drawn(cell_ids // NG % NG)
    freq_z = signed_freq_drawn(cell_ids % NG)

    def pick_cells(block_key, block_num):
        freq_x = signed_freq_drawn(block_num + block_count * plane_num)
        radius_sq = freq_x * freq_x + freq_y * freq_y + freq_z * freq_z
        jitter_key, order_key = jax.random.split(block_key)
        jitter_score = radius_sq * 8 + jax.random.randint(jitter_key, (slab_cells,), 0, 192, dtype=jnp.int32)
        chosen = jnp.argsort(jitter_score, stable=True)[:PW_DEV]
        shuffle = jax.random.permutation(order_key, PW_DEV)
        return chosen[shuffle].astype(jnp.int32)
    block_keys = jax.random.split(key, block_count)
    block_nums = jnp.arange(block_count, dtype=jnp.int32)
    return jax.vmap(pick_cells)(block_keys, block_nums).reshape(NPW)


def cell_energy(cells):
    block_count = NPW // PW_DEV
    owner = jnp.arange(NPW, dtype=jnp.int32) // PW_DEV
    freq_x = signed_freq_drawn(owner + block_count * (cells // (NG * NG)))
    freq_y = signed_freq_drawn(cells // NG % NG)
    freq_z = signed_freq_drawn(cells % NG)
    return kin_unit * (freq_x * freq_x + freq_y * freq_y + freq_z * freq_z).astype(jnp.float32)


def projector_values(key):
    cells = sphere_cells(jax.random.fold_in(key, 11))
    energy = cell_energy(cells)
    shape_key, scale_key = jax.random.split(jax.random.fold_in(key, 23))
    raw_values = jax.random.truncated_normal(shape_key, -6.0, 6.0, (2, NPROJ, NPW), jnp.float32)
    row_scale = jnp.exp(jax.random.uniform(scale_key, (NPROJ,), jnp.float32, -0.7, 0.7))
    shaped = raw_values * row_scale[None, :, None] / (1.0 + energy / 8.0)[None, None, :]
    return (jnp.clip(shaped, -6.0, 6.0), energy)


def draw_cell_map(key, part):
    return sphere_cells(jax.random.fold_in(key, 11))


def draw_projectors(key, part):
    return projector_values(key)[0]


def draw_coeffs(key, part):
    projectors, energy = projector_values(key)
    noise_key, mix_key, common_key, scale_key = jax.random.split(jax.random.fold_in(key, 37), 4)
    envelope = 1.0 / (1.0 + energy / 4.0)
    noise = jax.random.truncated_normal(noise_key, -6.0, 6.0, (2, NBANDS, NPW), jnp.float32)
    mixing = jax.random.truncated_normal(mix_key, -4.0, 4.0, (2, NBANDS, NPROJ), jnp.float32) * (0.5 / NPROJ ** 0.5)
    along_re = jnp.einsum('bp,pg->bg', mixing[0], projectors[0]) - jnp.einsum('bp,pg->bg', mixing[1], projectors[1])
    along_im = jnp.einsum('bp,pg->bg', mixing[0], projectors[1]) + jnp.einsum('bp,pg->bg', mixing[1], projectors[0])
    values = noise * envelope[None, None, :] + jnp.stack([along_re, along_im])
    return jnp.clip(values, -8.0, 8.0)


def projector_slots(key):
    ordering = jax.random.permutation(jax.random.fold_in(key, 51), NPROJ).astype(jnp.int32)
    return (ordering // NCH, ordering % NCH)


def draw_proj_atom(key, part):
    return projector_slots(key)[0]


def draw_proj_chan(key, part):
    return projector_slots(key)[1]


def shard_levels(key, extent, cuts, low, top_value):
    loudness = 1.0
    for axis_at, shards_of in cuts:
        heights = jax.random.uniform(jax.random.fold_in(jax.random.fold_in(key, 6), axis_at), (shards_of,), jnp.float32, low / len(cuts), top_value / len(cuts))
        loudness = loudness * jnp.repeat(jnp.exp(heights), extent[axis_at] // shards_of).reshape((-1,) + (1,) * (len(extent) - 1 - axis_at))
    return loudness


def setup_inputs(seed: int = 0) -> dict:
    arg_keys = jax.random.split(jax.random.key(seed), 8)
    coeffs = draw_coeffs(jax.random.fold_in(arg_keys[7], 71), 0)
    cell_map = draw_cell_map(jax.random.fold_in(arg_keys[7], 71), 0)
    potential = jnp.clip(-2.0 + 3.0 * jax.random.uniform(arg_keys[2], (NG, NG, NG), jnp.float32) ** shard_levels(arg_keys[2], (NG, NG, NG), ((1, 8),), -0.2, 0.2), -2.0, 1.0)
    projectors = draw_projectors(jax.random.fold_in(arg_keys[7], 71), 0)
    strengths = jnp.clip(jax.random.uniform(arg_keys[4], (NATOM, NCH, NCH), jnp.float32, -2.0, 2.0), -2.0, 2.0)
    proj_atom = draw_proj_atom(jax.random.fold_in(arg_keys[7], 71), 0)
    proj_chan = draw_proj_chan(jax.random.fold_in(arg_keys[7], 71), 0)
    return dict(coeffs=coeffs, cell_map=cell_map, potential=potential, projectors=projectors, strengths=strengths, proj_atom=proj_atom, proj_chan=proj_chan)


top_precision = lax.Precision.HIGHEST
kin_unit = 0.02
small_eps = 1e-6


def signed_freq(index_arr):
    return jnp.where(index_arr < NG // 2, index_arr, index_arr - NG)


def coupling_matrix(proj_atom, proj_chan, strengths):
    symmetric = 0.5 * (strengths + jnp.swapaxes(strengths, 1, 2))
    atom_hot = (proj_atom[:, None] == jnp.arange(NATOM, dtype=jnp.int32)[None, :]).astype(jnp.float32)
    chan_hot = (proj_chan[:, None] == jnp.arange(NCH, dtype=jnp.int32)[None, :]).astype(jnp.float32)
    rows_d = jnp.einsum("pa,pc,acd->pd", atom_hot, chan_hot, symmetric, precision=top_precision)
    same_atom = jnp.dot(atom_hot, atom_hot.T, precision=top_precision, preferred_element_type=jnp.float32)
    return same_atom * jnp.dot(rows_d, chan_hot.T, precision=top_precision, preferred_element_type=jnp.float32)


def band_dot(left_vec, right_vec, weight):
    return jnp.sum(left_vec * right_vec * weight, axis=(0, 2)) / NPW


def per_band(values):
    return values[None, :, None]


def precondition(residual, kinetic, kin_level):
    x_ratio = kinetic[None, :] / (1.5 * kin_level[:, None] + 1.0)
    numer_poly = 27.0 + x_ratio * (18.0 + x_ratio * (12.0 + 8.0 * x_ratio))
    square = x_ratio * x_ratio
    return residual * (numer_poly / (numer_poly + 16.0 * square * square))[None]


def pair_products(left_vec, right_vec):
    def contract(first_part, second_part):
        return jnp.einsum("bg,cg->bc", first_part, second_part, precision=top_precision)
    real_part = contract(left_vec[0], right_vec[0]) + contract(left_vec[1], right_vec[1])
    imag_part = contract(left_vec[0], right_vec[1]) - contract(left_vec[1], right_vec[0])
    return jnp.stack([real_part, imag_part])


def local_one(vector, flat_cells, potential):
    values = vector[0] + 1j * vector[1]
    grid_g = jnp.zeros((NG * NG * NG,), values.dtype).at[flat_cells].set(values)
    space = jnp.fft.ifftn(grid_g.reshape(NG, NG, NG)) * potential
    back = jnp.fft.fftn(space).reshape(NG * NG * NG)[flat_cells]
    return jnp.stack([jnp.real(back), jnp.imag(back)])


def reference(coeffs, cell_map, potential, projectors, strengths, proj_atom, proj_chan):
    owner = jnp.arange(NPW, dtype=jnp.int32) // PW_DEV
    x_index = owner + PW_BLOCKS * (cell_map // (NG * NG))
    y_index = (cell_map // NG) % NG
    z_index = cell_map % NG
    flat_cells = (x_index * NG + y_index) * NG + z_index
    freq_x = signed_freq(x_index)
    freq_y = signed_freq(y_index)
    freq_z = signed_freq(z_index)
    kinetic = kin_unit * (freq_x * freq_x + freq_y * freq_y + freq_z * freq_z).astype(jnp.float32)
    kin_weight = kinetic[None, None, :]
    coupling = coupling_matrix(proj_atom, proj_chan, strengths)

    def contract(first_part, second_part):
        return jnp.einsum("pg,bg->pb", first_part, second_part, precision=top_precision)

    def spread(weights, proj_table):
        return jnp.einsum("pb,pg->bg", weights, proj_table, precision=top_precision)

    def apply_h(vectors):
        local_term = lax.map(lambda vector: local_one(vector, flat_cells, potential), jnp.swapaxes(vectors, 0, 1))
        local_term = jnp.swapaxes(local_term, 0, 1)
        proj_re = (contract(projectors[0], vectors[0]) + contract(projectors[1], vectors[1])) / NPW
        proj_im = (contract(projectors[0], vectors[1]) - contract(projectors[1], vectors[0])) / NPW
        mixed_re = jnp.dot(coupling, proj_re, precision=top_precision, preferred_element_type=jnp.float32)
        mixed_im = jnp.dot(coupling, proj_im, precision=top_precision, preferred_element_type=jnp.float32)
        out_re = spread(mixed_re, projectors[0]) - spread(mixed_im, projectors[1])
        out_im = spread(mixed_re, projectors[1]) + spread(mixed_im, projectors[0])
        return kin_weight * vectors + local_term + jnp.stack([out_re, out_im])

    h_zero = apply_h(coeffs)
    eps_zero = band_dot(coeffs, h_zero, 1.0) / (band_dot(coeffs, coeffs, 1.0) + small_eps)
    r_zero = h_zero - per_band(eps_zero) * coeffs
    level_zero = band_dot(r_zero, r_zero, kin_weight) / (band_dot(r_zero, r_zero, 1.0) + small_eps)
    p_zero = precondition(r_zero, kinetic, level_zero)
    g_zero = apply_h(p_zero)
    q_zero = g_zero - per_band(eps_zero) * p_zero
    lam_zero = -band_dot(r_zero, q_zero, 1.0) / (band_dot(q_zero, q_zero, 1.0) + small_eps)
    psi_one = coeffs + per_band(lam_zero) * p_zero
    h_one = h_zero + per_band(lam_zero) * g_zero
    eps_one = band_dot(psi_one, h_one, 1.0) / (band_dot(psi_one, psi_one, 1.0) + small_eps)
    r_one = h_one - per_band(eps_one) * psi_one
    change = r_zero - r_one
    weight_one = band_dot(r_zero, change, 1.0) / (band_dot(change, change, 1.0) + small_eps)
    step_mid = weight_one * lam_zero
    psi_mid = coeffs + per_band(step_mid) * p_zero
    h_mid = h_zero + per_band(step_mid) * g_zero
    r_mid = r_zero - per_band(weight_one) * change
    eps_mid = band_dot(psi_mid, h_mid, 1.0) / (band_dot(psi_mid, psi_mid, 1.0) + small_eps)
    level_mid = band_dot(r_mid, r_mid, kin_weight) / (band_dot(r_mid, r_mid, 1.0) + small_eps)
    p_one = precondition(r_mid, kinetic, level_mid)
    g_one = apply_h(p_one)
    q_one = g_one - per_band(eps_mid) * p_one
    lam_one = -band_dot(r_mid, q_one, 1.0) / (band_dot(q_one, q_one, 1.0) + small_eps)
    new_bands = psi_mid + per_band(lam_one) * p_one
    new_ham = h_mid + per_band(lam_one) * g_one
    norm_new = band_dot(new_bands, new_bands, 1.0) + small_eps
    energy = band_dot(new_bands, new_ham, 1.0) / norm_new
    residual = new_ham - per_band(energy) * new_bands
    residual_norm = band_dot(residual, residual, 1.0) / norm_new
    correlation = pair_products(new_bands, new_bands) / NPW
    subspace = pair_products(new_bands, new_ham) / NPW
    return new_bands, energy, residual_norm, correlation, subspace
```

```python
import functools

import jax
import jax.numpy as jnp
import numpy as np
from jax import lax
from jax.experimental import pallas as pl
from jax.experimental.pallas import tpu as pltpu
from jax.sharding import PartitionSpec as P

top_precision = lax.Precision.HIGHEST
kin_unit = 0.02
small_eps = 1e-06


def signed_freq(index_arr, grid_len):
    return jnp.where(index_arr < grid_len // 2, index_arr, index_arr - grid_len)


def wave_tables(grid_len, row_freq, col_freq, sign_val, factor):
    phase = row_freq[:, None] * col_freq[None, :] % grid_len
    angle = 2.0 * jnp.pi / grid_len * phase.astype(jnp.float32)
    return (jnp.cos(angle) * factor, jnp.sin(angle) * (sign_val * factor))


def block_table(cos_table, sin_table):
    upper = jnp.concatenate([cos_table, sin_table], axis=1)
    lower = jnp.concatenate([-sin_table, cos_table], axis=1)
    return jnp.concatenate([upper, lower], axis=0)


def quarter_turn(grid_vals):
    half_len = grid_vals.shape[-1] // 2
    return jnp.concatenate([-grid_vals[..., half_len:], grid_vals[..., :half_len]], axis=-1)


def mix_dim(grid_vals, cos_table, sin_table, pattern):
    direct = jnp.einsum(pattern, cos_table, grid_vals, precision=top_precision)
    turned = jnp.einsum(pattern, sin_table, quarter_turn(grid_vals), precision=top_precision)
    return direct + turned


def mix_last(grid_vals, table_full):
    row_width = grid_vals.shape[-1]
    product = jnp.dot(
        grid_vals.reshape(-1, row_width),
        table_full,
        precision=top_precision,
        preferred_element_type=jnp.float32,
    )
    return product.reshape(grid_vals.shape)


def band_dot(left_vec, right_vec, weight):
    return jnp.sum(left_vec * right_vec * weight, axis=(0, 2))


def per_band(values):
    return values[None, :, None]


def pair_products(left_vec, right_vec):

    def contract(first_part, second_part):
        return jnp.einsum("bg,cg->bc", first_part, second_part, precision=top_precision)

    real_part = contract(left_vec[0], right_vec[0]) + contract(left_vec[1], right_vec[1])
    imag_part = contract(left_vec[0], right_vec[1]) - contract(left_vec[1], right_vec[0])
    return jnp.stack([real_part, imag_part])


def precondition(residual, kinetic, kin_level):
    x_ratio = kinetic[None, :] / (1.5 * kin_level[:, None] + 1.0)
    numer_poly = 27.0 + x_ratio * (18.0 + x_ratio * (12.0 + 8.0 * x_ratio))
    square = x_ratio * x_ratio
    return residual * (numer_poly / (numer_poly + 16.0 * square * square))[None]


def coupling_matrix(proj_atom, proj_chan, strengths):
    atom_count = strengths.shape[0]
    chan_count = strengths.shape[1]
    symmetric = 0.5 * (strengths + jnp.swapaxes(strengths, 1, 2))
    atom_hot = (proj_atom[:, None] == jnp.arange(atom_count, dtype=jnp.int32)[None, :]).astype(
        jnp.float32
    )
    chan_hot = (proj_chan[:, None] == jnp.arange(chan_count, dtype=jnp.int32)[None, :]).astype(
        jnp.float32
    )
    rows_d = jnp.einsum("pa,pc,acd->pd", atom_hot, chan_hot, symmetric, precision=top_precision)
    same_atom = jnp.dot(
        atom_hot, atom_hot.T, precision=top_precision, preferred_element_type=jnp.float32
    )
    return same_atom * jnp.dot(
        rows_d, chan_hot.T, precision=top_precision, preferred_element_type=jnp.float32
    )


def combine(term_list):
    merged = {}
    for scalar, coef_map in term_list:
        for index_one, coef_a in coef_map.items():
            merged[index_one] = merged.get(index_one, 0.0) + scalar * coef_a
    return merged


def gram_form(gram_table, left_map, right_map, use_kin):
    running = 0.0
    for index_one, coef_a in left_map.items():
        for index_two, coef_b in right_map.items():
            running = running + coef_a * coef_b * gram_table[use_kin, index_one, index_two]
    return running


def new_pairs(first_new, last_new, kinds):
    pair_list = []
    for use_kin in kinds:
        for index_two in range(first_new, last_new):
            for index_one in range(index_two + 1):
                pair_list.append((index_one, index_two, use_kin))
    return pair_list


def plain_body(coeffs, cell_map, potential, projectors, strengths, proj_atom, proj_chan):
    ga_count = lax.axis_size("ga")
    grid_len = potential.shape[0]
    planes = grid_len // ga_count
    band_local = coeffs.shape[1]
    total_pw = coeffs.shape[2] * ga_count
    device = lax.axis_index("ga")
    plane_num = cell_map // (grid_len * grid_len)
    y_index = cell_map // grid_len % grid_len
    z_index = cell_map % grid_len
    freq_x = signed_freq(device + ga_count * plane_num, grid_len)
    freq_y = signed_freq(y_index, grid_len)
    freq_z = signed_freq(z_index, grid_len)
    kinetic = kin_unit * (freq_x * freq_x + freq_y * freq_y + freq_z * freq_z).astype(jnp.float32)
    kin_weight = kinetic[None, None, :]
    slot_re = (plane_num * grid_len + y_index) * (2 * grid_len) + z_index
    slot_im = slot_re + grid_len
    cell_count = planes * grid_len * 2 * grid_len
    natural = jnp.arange(grid_len, dtype=jnp.int32)
    cyclic = natural % planes * ga_count + natural // planes
    cos_fwd, sin_fwd = wave_tables(grid_len, natural, natural, 1.0, 1.0)
    cos_back, sin_back = wave_tables(grid_len, natural, natural, -1.0, 1.0 / grid_len)
    z_forward = block_table(cos_fwd, sin_fwd)
    z_backward = block_table(cos_back, sin_back)
    xcos_fwd, xsin_fwd = wave_tables(grid_len, natural, cyclic, 1.0, 1.0)
    xcos_back, xsin_back = wave_tables(grid_len, cyclic, natural, -1.0, 1.0 / grid_len)
    doubled = jnp.concatenate([potential, potential], axis=-1)
    coupling = coupling_matrix(proj_atom, proj_chan, strengths)

    def real_space(grid_vals):
        grid_vals = mix_dim(grid_vals, xcos_fwd, xsin_fwd, "kj,bjyw->bkyw")
        grid_vals = grid_vals * doubled[None]
        grid_vals = mix_dim(grid_vals, xcos_back, xsin_back, "jk,bkyw->bjyw")
        return lax.all_to_all(grid_vals, "ga", split_axis=1, concat_axis=2, tiled=True)

    def local_part(vectors):
        item_count = vectors.shape[1]
        flat_grid = jnp.zeros((item_count, cell_count), jnp.float32)
        flat_grid = flat_grid.at[:, slot_re].set(vectors[0]).at[:, slot_im].set(vectors[1])
        grid_vals = mix_last(
            flat_grid.reshape(item_count, planes, grid_len, 2 * grid_len), z_forward
        )
        grid_vals = mix_dim(grid_vals, cos_fwd, sin_fwd, "ky,bpyw->bpkw")
        grid_vals = real_space(
            lax.all_to_all(grid_vals, "ga", split_axis=2, concat_axis=1, tiled=True)
        )
        grid_vals = mix_dim(grid_vals, cos_back, sin_back, "ky,bpyw->bpkw")
        flat_grid = mix_last(grid_vals, z_backward).reshape(item_count, cell_count)
        return jnp.stack([flat_grid[:, slot_re], flat_grid[:, slot_im]])

    def contract(first_part, second_part):
        return jnp.einsum("pg,bg->pb", first_part, second_part, precision=top_precision)

    def spread(weights, proj_table):
        return jnp.einsum("pb,pg->bg", weights, proj_table, precision=top_precision)

    def projected_part(vectors):
        proj_re = contract(projectors[0], vectors[0]) + contract(projectors[1], vectors[1])
        proj_im = contract(projectors[0], vectors[1]) - contract(projectors[1], vectors[0])
        proj_re, proj_im = lax.psum((proj_re, proj_im), "ga")
        mixed_re = jnp.dot(
            coupling,
            proj_re / total_pw,
            precision=top_precision,
            preferred_element_type=jnp.float32,
        )
        mixed_im = jnp.dot(
            coupling,
            proj_im / total_pw,
            precision=top_precision,
            preferred_element_type=jnp.float32,
        )
        out_re = spread(mixed_re, projectors[0]) - spread(mixed_im, projectors[1])
        out_im = spread(mixed_re, projectors[1]) + spread(mixed_im, projectors[0])
        return jnp.stack([out_re, out_im])

    def apply_h(vectors):
        return kin_weight * vectors + local_part(vectors) + projected_part(vectors)

    def gram_sums(basis, pair_list):
        stacked = []
        for index_one, index_two, use_kin in pair_list:
            stacked.append(
                band_dot(basis[index_one], basis[index_two], kin_weight if use_kin else 1.0)
            )
        summed = lax.psum(jnp.stack(stacked), "ga") / total_pw
        found = {}
        for slot_num, entry in enumerate(pair_list):
            index_one, index_two, use_kin = entry
            found[use_kin, index_one, index_two] = summed[slot_num]
            found[use_kin, index_two, index_one] = summed[slot_num]
        return found

    def realize(coef_map, basis):
        running = jnp.zeros_like(basis[0])
        for index_one, coef_a in coef_map.items():
            running = (
                running
                + per_band(jnp.zeros((band_local,), jnp.float32) + coef_a) * basis[index_one]
            )
        return running

    h_zero = apply_h(coeffs)
    basis = [coeffs, h_zero]
    gram_table = gram_sums(basis, new_pairs(0, 2, (False, True)))
    psi_map = {0: 1.0}
    ham_map = {1: 1.0}
    eps_zero = gram_form(gram_table, psi_map, ham_map, False) / (
        gram_form(gram_table, psi_map, psi_map, False) + small_eps
    )
    r_map = combine([(1.0, ham_map), (-eps_zero, psi_map)])
    level_zero = gram_form(gram_table, r_map, r_map, True) / (
        gram_form(gram_table, r_map, r_map, False) + small_eps
    )
    p_zero = precondition(realize(r_map, basis), kinetic, level_zero)
    g_zero = apply_h(p_zero)
    basis = [coeffs, h_zero, p_zero, g_zero]
    gram_table.update(gram_sums(basis, new_pairs(2, 4, (False, True))))
    q_map = combine([(1.0, {3: 1.0}), (-eps_zero, {2: 1.0})])
    lam_zero = -gram_form(gram_table, r_map, q_map, False) / (
        gram_form(gram_table, q_map, q_map, False) + small_eps
    )
    psi_one_map = combine([(1.0, psi_map), (lam_zero, {2: 1.0})])
    h_one_map = combine([(1.0, ham_map), (lam_zero, {3: 1.0})])
    eps_one = gram_form(gram_table, psi_one_map, h_one_map, False) / (
        gram_form(gram_table, psi_one_map, psi_one_map, False) + small_eps
    )
    r_one_map = combine([(1.0, h_one_map), (-eps_one, psi_one_map)])
    change_map = combine([(1.0, r_map), (-1.0, r_one_map)])
    weight_one = gram_form(gram_table, r_map, change_map, False) / (
        gram_form(gram_table, change_map, change_map, False) + small_eps
    )
    step_mid = weight_one * lam_zero
    psi_mid_map = combine([(1.0, psi_map), (step_mid, {2: 1.0})])
    h_mid_map = combine([(1.0, ham_map), (step_mid, {3: 1.0})])
    r_mid_map = combine([(1.0, r_map), (-weight_one, change_map)])
    eps_mid = gram_form(gram_table, psi_mid_map, h_mid_map, False) / (
        gram_form(gram_table, psi_mid_map, psi_mid_map, False) + small_eps
    )
    level_mid = gram_form(gram_table, r_mid_map, r_mid_map, True) / (
        gram_form(gram_table, r_mid_map, r_mid_map, False) + small_eps
    )
    p_one = precondition(realize(r_mid_map, basis), kinetic, level_mid)
    g_one = apply_h(p_one)
    basis = [coeffs, h_zero, p_zero, g_zero, p_one, g_one]
    gram_table.update(gram_sums(basis, new_pairs(4, 6, (False,))))
    q_one_map = combine([(1.0, {5: 1.0}), (-eps_mid, {4: 1.0})])
    lam_one = -gram_form(gram_table, r_mid_map, q_one_map, False) / (
        gram_form(gram_table, q_one_map, q_one_map, False) + small_eps
    )
    new_map = combine([(1.0, psi_mid_map), (lam_one, {4: 1.0})])
    ham_new_map = combine([(1.0, h_mid_map), (lam_one, {5: 1.0})])
    norm_new = gram_form(gram_table, new_map, new_map, False) + small_eps
    energy = gram_form(gram_table, new_map, ham_new_map, False) / norm_new
    resid_map = combine([(1.0, ham_new_map), (-energy, new_map)])
    residual_norm = gram_form(gram_table, resid_map, resid_map, False) / norm_new
    new_bands = realize(new_map, basis)
    new_ham = realize(ham_new_map, basis)
    blank_rows = jnp.zeros((2, band_local, band_local * lax.axis_size("band")), jnp.float32)
    first_row = jnp.int32(0)
    over_rows = blank_rows
    ham_rows = blank_rows
    piece_bands = lax.all_gather(new_bands, "band", axis=1, tiled=True)
    piece_ham = lax.all_gather(new_ham, "band", axis=1, tiled=True)
    over_rows = lax.dynamic_update_slice_in_dim(
        over_rows, pair_products(new_bands, piece_bands), first_row, 2
    )
    ham_rows = lax.dynamic_update_slice_in_dim(
        ham_rows, pair_products(new_bands, piece_ham), first_row, 2
    )
    over_rows, ham_rows = (over_rows, ham_rows)
    over_rows, ham_rows = lax.psum((over_rows, ham_rows), "ga")
    correlation = over_rows / total_pw
    subspace = ham_rows / total_pw
    return (new_bands, energy, residual_norm, correlation, subspace)


QUAD = 4
TRIPLE = 3
MESH = pl.DeviceIdType.MESH


def split_const(values):
    high = np.asarray(values, np.float32).astype(jnp.bfloat16)
    low = (values - high.astype(np.float64)).astype(np.float32).astype(jnp.bfloat16)
    return np.stack([high, low])


def const_tables(grid_len, group):
    planes = grid_len // group
    chunks = planes // QUAD
    unit = 2.0 * np.pi / grid_len
    quarter = grid_len / 4.0
    chunk = np.arange(chunks)[:, None, None, None]
    dev = np.arange(group)[None, :, None, None]
    part = np.arange(2)[None, None, :, None]
    inner = np.arange(QUAD)[None, None, None, :]
    y_real = (dev * planes + chunk * QUAD + inner + 0 * part).reshape(-1)
    part_row = (part + 0 * (dev + chunk + inner)).reshape(-1)
    freq = np.arange(grid_len)
    phase = (y_real[:, None] * freq[None, :]) % grid_len
    tab_a = np.cos(unit * (phase - quarter * part_row[:, None]))
    tab_b = np.cos(unit * (phase + quarter * (1 - part_row[:, None])))
    wave = split_const(np.concatenate([tab_a, tab_b], axis=0))
    four = np.repeat(np.arange(4), grid_len)
    zed = np.tile(freq, 4)
    theta = 2.0 * np.pi * ((four[:, None] * four[None, :] % 4) / 4.0
                           + (zed[:, None] * zed[None, :] % grid_len) / grid_len)
    fourz = split_const(np.concatenate([np.cos(theta), np.sin(theta)], axis=1))
    dft = 2.0 * np.pi * np.outer(np.arange(group), np.arange(group)) / group
    real_mix = np.zeros((group, 2, QUAD, group, 2, QUAD))
    for row in range(QUAD):
        real_mix[:, 0, row, :, 0, row] = np.cos(dft)
        real_mix[:, 1, row, :, 1, row] = np.cos(dft)
        real_mix[:, 0, row, :, 1, row] = -np.sin(dft)
        real_mix[:, 1, row, :, 0, row] = np.sin(dft)
    size = group * 2 * QUAD
    real_mix = real_mix.reshape(size, size)

    def stacked(mat):
        high, low = split_const(mat)
        return np.concatenate([high, high, low], axis=1)

    across = np.stack([stacked(real_mix), stacked(real_mix.T)])
    b_lane = np.repeat(np.arange(TRIPLE), 4 * grid_len)
    a_lane = np.tile(np.repeat(np.arange(4), grid_len), TRIPLE)
    one = 2.0 * np.pi * (a_lane * b_lane) / planes
    two = unit * np.outer(np.arange(group), TRIPLE * a_lane + b_lane)
    lane_tw = np.stack([np.cos(one), np.sin(one)]).astype(np.float32)[:, None, :]
    dev_tw = np.stack([np.cos(two), np.sin(two)]).astype(np.float32)[:, :, None, :]
    return wave, fourz, across, lane_tw, dev_tw


def two_parts(values):
    high = values.astype(jnp.bfloat16)
    low = (values - high.astype(jnp.float32)).astype(jnp.bfloat16)
    return high, low


def bdot(left, right):
    return jnp.dot(left, right, preferred_element_type=jnp.float32)


def sweep_kernel(
    dims,
    coeffs_ref, kin_ref, ynum_ref, key_row_ref, key_col_ref, pot_ref, proj_ref, coup_ref,
    wave_ref, fourz_ref, across_ref, lane_ref, dev_ref,
    new_ref, scal_ref,
    hot_ref, hot_t_ref, ta_ref, tb_ref,
    fsend, frecv, bsend, brecv, psend, precv, gsend, grecv, nsend, nrecv, csend, crecv,
    fs_sem, fr_sem, bs_sem, br_sem, ps_sem, pr_sem, gs_sem, gr_sem, ns_sem, nr_sem, cs_sem, cr_sem,
):
    group, bands, chunks, grid_len, total_pw, pw = dims
    rows = group * 2 * QUAD
    lanes = TRIPLE * 4 * grid_len
    quad_lanes = 4 * grid_len
    me = lax.axis_index("ga")
    band = lax.axis_index("band")

    barrier = pltpu.get_barrier_semaphore()
    for off in range(1, group):
        pl.semaphore_signal(barrier, inc=1, device_id={"ga": lax.rem(me + off, group)}, device_id_type=MESH)
    for off in range(1, bands):
        pl.semaphore_signal(barrier, inc=1, device_id={"band": lax.rem(band + off, bands)}, device_id_type=MESH)

    hot_rows = 256

    def build_hot(step, carry):
        at = pl.multiple_of(step * hot_rows, hot_rows)
        lane_id = lax.broadcasted_iota(jnp.int32, (hot_rows, lanes), 1)
        hot_ref[pl.ds(at, hot_rows), :] = (lane_id == key_col_ref[pl.ds(at, hot_rows), :]).astype(jnp.float32).astype(jnp.bfloat16)
        return carry

    lax.fori_loop(0, pw // hot_rows, build_hot, 0)
    turn_rows = 128

    def build_turn(step, carry):
        at = pl.multiple_of(step * turn_rows, turn_rows)
        row_id = lax.broadcasted_iota(jnp.int32, (turn_rows, pw), 0) + at
        hot_t_ref[pl.ds(at, turn_rows), :] = (row_id == key_row_ref[...]).astype(jnp.float32).astype(jnp.bfloat16)
        return carry

    lax.fori_loop(0, lanes // turn_rows, build_turn, 0)
    y_hot = (lax.broadcasted_iota(jnp.int32, (grid_len, pw), 0) == ynum_ref[...]).astype(jnp.float32).astype(jnp.bfloat16)
    for part in range(chunks):
        for table, base in ((ta_ref, 0), (tb_ref, chunks * rows)):
            at = base + part * rows
            table[part] = bdot(wave_ref[0, at:at + rows, :], y_hot) + bdot(wave_ref[1, at:at + rows, :], y_hot)

    pl.semaphore_wait(barrier, group + bands - 2)

    kin = kin_ref[...]
    sign = jnp.where(lax.broadcasted_iota(jnp.int32, (1, 2 * QUAD, 1), 1) < QUAD, -1.0, 1.0).astype(jnp.float32)

    def times_i(values):
        return pltpu.roll(values, QUAD, 1) * sign

    def lane_split(values):
        return [values[..., k * quad_lanes:(k + 1) * quad_lanes] for k in range(TRIPLE)]

    def mix_fourz(triple, direction):
        stacked = jnp.concatenate([t.reshape(rows, quad_lanes) for t in triple], axis=0)
        high, low = two_parts(stacked)
        out = bdot(high, fourz_ref[0]) + bdot(low, fourz_ref[0]) + bdot(high, fourz_ref[1])
        out = out.reshape(TRIPLE * group, 2 * QUAD, 2 * quad_lanes)
        mixed = out[..., :quad_lanes] + direction * times_i(out[..., quad_lanes:])
        return [mixed[k * group:(k + 1) * group] for k in range(TRIPLE)]

    def turn_lane(triple, direction):
        done = [triple[0]]
        for k in range(1, TRIPLE):
            at = slice(k * quad_lanes, (k + 1) * quad_lanes)
            done.append(triple[k] * lane_ref[0, :, at][None] + direction * times_i(triple[k]) * lane_ref[1, :, at][None])
        return done

    def three(triple, direction):
        total = triple[1] + triple[2]
        diff = times_i(triple[1] - triple[2]) * (direction * 0.8660254037844386)
        base = triple[0] - 0.5 * total
        return [triple[0] + total, base + diff, base - diff]

    def turn_dev(values, direction):
        return values * dev_ref[0] + direction * times_i(values) * dev_ref[1]

    def mix_devices(values, which):
        high, low = two_parts(values.reshape(rows, lanes))
        return bdot(across_ref[which], jnp.concatenate([high, low, high], axis=0))

    def all_sum(local, send, recv, send_sem, recv_sem, shape_at):
        send[shape_at] = local
        recv[shape_at, me] = local
        for off in range(1, group):
            pltpu.make_async_remote_copy(
                src_ref=send.at[shape_at], dst_ref=recv.at[shape_at, me],
                send_sem=send_sem.at[shape_at, off - 1], recv_sem=recv_sem.at[shape_at, off - 1],
                device_id={"ga": lax.rem(me + off, group)}, device_id_type=MESH).start()

    def all_sum_end(send, recv, send_sem, recv_sem, shape_at):
        for off in range(1, group):
            pltpu.make_async_remote_copy(
                src_ref=send.at[shape_at], dst_ref=recv.at[shape_at, lax.rem(me + group - off, group)],
                send_sem=send_sem.at[shape_at, off - 1], recv_sem=recv_sem.at[shape_at, off - 1],
                device_id={"ga": lax.rem(me + off, group)}, device_id_type=MESH).wait()
        running = recv[shape_at, 0]
        for dev in range(1, group):
            running = running + recv[shape_at, dev]
        return running

    def piece(turn, part, off, send, recv, send_sem, recv_sem, incoming):
        peer = lax.rem(me + off, group)
        source = lax.rem(me + group - off, group) if incoming else me
        return pltpu.make_async_remote_copy(
            src_ref=send.at[turn, part, peer], dst_ref=recv.at[turn, part, source],
            send_sem=send_sem.at[turn, part, off - 1], recv_sem=recv_sem.at[turn, part, off - 1],
            device_id={"ga": peer}, device_id_type=MESH)

    def apply_h(turn, vector):
        v_re, v_im = vector[0:1], vector[1:2]
        fwd = (fsend, frecv, fs_sem, fr_sem)
        back = (bsend, brecv, bs_sem, br_sem)

        def put(part, carry):
            high, low = two_parts(ta_ref[part] * v_re + tb_ref[part] * v_im)
            out = bdot(jnp.concatenate([high, low], axis=0), hot_ref[...])
            out = (out[:rows] + out[rows:]).reshape(group, 2 * QUAD, lanes)
            fsend[turn, part] = out
            frecv[turn, part, me] = fsend[turn, part, me]
            for off in range(1, group):
                piece(turn, part, off, *fwd, False).start()
            return carry

        lax.fori_loop(0, chunks, put, 0)
        sums = lax.dot_general(vector, proj_ref[...], (((1,), (1,)), ((), ())), precision=top_precision, preferred_element_type=jnp.float32)
        all_sum(sums, psend, precv, ps_sem, pr_sem, turn)

        def middle(part, carry):
            for off in range(1, group):
                piece(turn, part, off, *fwd, True).wait()
            triple = turn_lane(three(lane_split(frecv[turn, part]), 1.0), 1.0)
            values = turn_dev(jnp.concatenate(mix_fourz(triple, 1.0), axis=-1), 1.0)
            values = mix_devices(values, 0) * pot_ref[part]
            values = mix_devices(values, 1).reshape(group, 2 * QUAD, lanes)
            triple = mix_fourz(lane_split(turn_dev(values, -1.0)), -1.0)
            triple = three(turn_lane(triple, -1.0), -1.0)
            bsend[turn, part] = jnp.concatenate(triple, axis=-1)
            brecv[turn, part, me] = bsend[turn, part, me]
            for off in range(1, group):
                piece(turn, part, off, *back, False).start()
            return carry

        lax.fori_loop(0, chunks, middle, 0)
        sums = all_sum_end(psend, precv, ps_sem, pr_sem, turn) * (1.0 / total_pw)
        direct = jnp.dot(sums, coup_ref[0], precision=top_precision, preferred_element_type=jnp.float32)
        turned = jnp.dot(sums, coup_ref[1], precision=top_precision, preferred_element_type=jnp.float32)
        weights = jnp.concatenate([direct[0:1] + turned[1:2], direct[1:2] - turned[0:1]], axis=0)
        nonlocal_part = jnp.dot(weights, proj_ref[...], precision=top_precision, preferred_element_type=jnp.float32)
        start = kin * vector + nonlocal_part

        def take(part, carry):
            run_re, run_im = carry
            for off in range(1, group):
                piece(turn, part, off, *back, True).wait()
            high, low = two_parts(brecv[turn, part].reshape(rows, lanes))
            out = bdot(jnp.concatenate([high, low], axis=0), hot_t_ref[...])
            out = out[:rows] + out[rows:]
            run_re = run_re + jnp.sum(ta_ref[part] * out, axis=0, keepdims=True)
            run_im = run_im + jnp.sum(tb_ref[part] * out, axis=0, keepdims=True)
            return run_re, run_im

        run_re, run_im = lax.fori_loop(0, chunks, take, (start[0:1], start[1:2]))
        return jnp.concatenate([run_re, run_im], axis=0)

    def as_row(values):
        total = jnp.sum(jnp.sum(values, axis=0, keepdims=True), axis=1, keepdims=True)
        return jnp.broadcast_to(total, (1, 128))

    row_count = gsend.shape[1]

    def gram_sums(turn, basis, pair_list):
        found_rows = []
        for one, two, use_kin in pair_list:
            product = basis[one] * basis[two]
            found_rows.append(as_row(product * kin if use_kin else product))
        found_rows += [jnp.zeros((1, 128), jnp.float32)] * (row_count - len(found_rows))
        all_sum(jnp.concatenate(found_rows, axis=0), gsend, grecv, gs_sem, gr_sem, turn)
        summed = all_sum_end(gsend, grecv, gs_sem, gr_sem, turn) * (1.0 / total_pw)
        found = {}
        for slot, (one, two, use_kin) in enumerate(pair_list):
            value = summed[slot:slot + 1]
            found[use_kin, one, two] = value
            found[use_kin, two, one] = value
        return found

    def realize(coef_map, basis):
        running = 0.0
        for index, coef in coef_map.items():
            running = running + (basis[index] if isinstance(coef, float) and coef == 1.0 else spread_row(coef) * basis[index])
        return running

    def spread_row(coef):
        return coef if isinstance(coef, float) else coef[:, 0:1]

    def smooth(residual, level):
        ratio = kin / (1.5 * level[:, 0:1] + 1.0)
        poly = 27.0 + ratio * (18.0 + ratio * (12.0 + 8.0 * ratio))
        square = ratio * ratio
        return residual * (poly / (poly + 16.0 * square * square))

    coeffs = coeffs_ref[...]
    h_zero = apply_h(0, coeffs)
    basis = [coeffs, h_zero]
    gram = gram_sums(0, basis, new_pairs(0, 2, (False, True)))
    psi = {0: 1.0}
    ham = {1: 1.0}
    eps_zero = gram_form(gram, psi, ham, False) / (gram_form(gram, psi, psi, False) + small_eps)
    r_map = combine([(1.0, ham), (-eps_zero, psi)])
    level = gram_form(gram, r_map, r_map, True) / (gram_form(gram, r_map, r_map, False) + small_eps)
    p_zero = smooth(realize(r_map, basis), level)
    g_zero = apply_h(1, p_zero)
    basis += [p_zero, g_zero]
    gram.update(gram_sums(1, basis, new_pairs(2, 4, (False, True))))
    q_map = combine([(1.0, {3: 1.0}), (-eps_zero, {2: 1.0})])
    lam_zero = -gram_form(gram, r_map, q_map, False) / (gram_form(gram, q_map, q_map, False) + small_eps)
    psi_one = combine([(1.0, psi), (lam_zero, {2: 1.0})])
    h_one = combine([(1.0, ham), (lam_zero, {3: 1.0})])
    eps_one = gram_form(gram, psi_one, h_one, False) / (gram_form(gram, psi_one, psi_one, False) + small_eps)
    r_one = combine([(1.0, h_one), (-eps_one, psi_one)])
    change = combine([(1.0, r_map), (-1.0, r_one)])
    weight = gram_form(gram, r_map, change, False) / (gram_form(gram, change, change, False) + small_eps)
    step = weight * lam_zero
    psi_mid = combine([(1.0, psi), (step, {2: 1.0})])
    h_mid = combine([(1.0, ham), (step, {3: 1.0})])
    r_mid = combine([(1.0, r_map), (-weight, change)])
    eps_mid = gram_form(gram, psi_mid, h_mid, False) / (gram_form(gram, psi_mid, psi_mid, False) + small_eps)
    level = gram_form(gram, r_mid, r_mid, True) / (gram_form(gram, r_mid, r_mid, False) + small_eps)
    p_one = smooth(realize(r_mid, basis), level)
    g_one = apply_h(2, p_one)
    basis += [p_one, g_one]
    gram.update(gram_sums(2, basis, new_pairs(4, 6, (False,))))
    q_one = combine([(1.0, {5: 1.0}), (-eps_mid, {4: 1.0})])
    lam_one = -gram_form(gram, r_mid, q_one, False) / (gram_form(gram, q_one, q_one, False) + small_eps)
    new_map = combine([(1.0, psi_mid), (lam_one, {4: 1.0})])
    ham_new = combine([(1.0, h_mid), (lam_one, {5: 1.0})])
    norm_new = gram_form(gram, new_map, new_map, False) + small_eps
    energy = gram_form(gram, new_map, ham_new, False) / norm_new
    resid = combine([(1.0, ham_new), (-energy, new_map)])
    resid_norm = gram_form(gram, resid, resid, False) / norm_new
    new = realize(new_map, basis)
    new_h = realize(ham_new, basis)
    new_ref[...] = new
    both = jnp.concatenate([new, new_h, jnp.zeros((4, pw), jnp.float32)], axis=0)
    nsend[...] = both
    nrecv[band] = both

    def swap(off, incoming):
        source = lax.rem(band + bands - off, bands) if incoming else band
        return pltpu.make_async_remote_copy(
            src_ref=nsend, dst_ref=nrecv.at[source], send_sem=ns_sem.at[off - 1], recv_sem=nr_sem.at[off - 1],
            device_id={"band": lax.rem(band + off, bands)}, device_id_type=MESH)

    for off in range(1, bands):
        swap(off, False).start()
    for off in range(1, bands):
        swap(off, True).wait()
    found_rows = []
    for first in (0, 2):
        for imag in (False, True):
            for other in range(bands):
                o_re = nrecv[other, first:first + 1]
                o_im = nrecv[other, first + 1:first + 2]
                if imag:
                    found_rows.append(as_row(new[0:1] * o_im - new[1:2] * o_re))
                else:
                    found_rows.append(as_row(new[0:1] * o_re + new[1:2] * o_im))
    all_sum(jnp.concatenate(found_rows, axis=0), csend, crecv, cs_sem, cr_sem, 0)
    summed = all_sum_end(csend, crecv, cs_sem, cr_sem, 0) * (1.0 / total_pw)
    scal_ref[...] = jnp.concatenate([summed, energy, resid_norm, jnp.zeros((6, 128), jnp.float32)], axis=0)


def kernel_body(coeffs, cell_map, potential, projectors, strengths, proj_atom, proj_chan):
    group = lax.axis_size("ga")
    bands = lax.axis_size("band")
    grid_len = potential.shape[0]
    planes = grid_len // group
    chunks = planes // QUAD
    pw = coeffs.shape[2]
    total_pw = pw * group
    device = lax.axis_index("ga")
    plane_num = cell_map // (grid_len * grid_len)
    y_index = cell_map // grid_len % grid_len
    z_index = cell_map % grid_len
    freq_x = signed_freq(device + group * plane_num, grid_len)
    freq_y = signed_freq(y_index, grid_len)
    freq_z = signed_freq(z_index, grid_len)
    kinetic = kin_unit * (freq_x * freq_x + freq_y * freq_y + freq_z * freq_z).astype(jnp.float32)
    key = plane_num * grid_len + z_index
    pot = (potential * (1.0 / grid_len**3)).reshape(group, 4, TRIPLE, chunks, QUAD, grid_len)
    pot = jnp.transpose(pot, (3, 0, 4, 2, 1, 5)).reshape(chunks, group, 1, QUAD, planes * grid_len)
    rows = group * 2 * QUAD
    lanes = planes * grid_len
    pot = jnp.broadcast_to(pot, (chunks, group, 2, QUAD, lanes)).reshape(chunks, rows, lanes)
    coupling = coupling_matrix(proj_atom, proj_chan, strengths)
    blank = jnp.zeros_like(coupling)
    coup = jnp.stack([
        jnp.block([[coupling, blank], [blank, coupling]]),
        jnp.block([[blank, -coupling], [coupling, blank]]),
    ])
    proj_rows = 2 * projectors.shape[1]
    tables = [jnp.asarray(t) for t in const_tables(grid_len, group)]
    gram_rows = 16
    piece_shape = (3, chunks, group, 2 * QUAD, lanes)
    dma = pltpu.SemaphoreType.DMA
    vmem = pl.BlockSpec(memory_space=pltpu.VMEM)
    f32 = jnp.float32
    new, scal = pl.pallas_call(
        functools.partial(sweep_kernel, (group, bands, chunks, grid_len, total_pw, pw)),
        out_shape=(
            jax.ShapeDtypeStruct((2, pw), f32),
            jax.ShapeDtypeStruct((4 * bands + 8, 128), f32),
        ),
        in_specs=[vmem] * 13,
        out_specs=(vmem, vmem),
        scratch_shapes=[
            pltpu.VMEM((pw, lanes), jnp.bfloat16),
            pltpu.VMEM((lanes, pw), jnp.bfloat16),
            pltpu.VMEM((chunks, rows, pw), f32),
            pltpu.VMEM((chunks, rows, pw), f32),
            pltpu.VMEM(piece_shape, f32),
            pltpu.VMEM(piece_shape, f32),
            pltpu.VMEM(piece_shape, f32),
            pltpu.VMEM(piece_shape, f32),
            pltpu.VMEM((3, 2, proj_rows), f32),
            pltpu.VMEM((3, group, 2, proj_rows), f32),
            pltpu.VMEM((3, gram_rows, 128), f32),
            pltpu.VMEM((3, group, gram_rows, 128), f32),
            pltpu.VMEM((8, pw), f32),
            pltpu.VMEM((bands, 8, pw), f32),
            pltpu.VMEM((1, 4 * bands, 128), f32),
            pltpu.VMEM((1, group, 4 * bands, 128), f32),
            dma((3, chunks, group - 1)), dma((3, chunks, group - 1)),
            dma((3, chunks, group - 1)), dma((3, chunks, group - 1)),
            dma((3, group - 1)), dma((3, group - 1)),
            dma((3, group - 1)), dma((3, group - 1)),
            dma((bands - 1,)), dma((bands - 1,)),
            dma((1, group - 1)), dma((1, group - 1)),
        ],
        compiler_params=pltpu.CompilerParams(
            collective_id=0, has_side_effects=True, vmem_limit_bytes=60 * 1024 * 1024
        ),
        name="sweeps",
    )(
        coeffs.reshape(2, pw), kinetic[None, :], y_index[None, :], key[None, :], key[:, None],
        pot, projectors.reshape(proj_rows, pw), coup, *tables,
    )
    rows_out = scal[: 4 * bands, 0].reshape(2, 2, 1, bands)
    return (
        new.reshape(2, 1, pw), scal[4 * bands, :1], scal[4 * bands + 1, :1], rows_out[0], rows_out[1],
    )


def body(coeffs, cell_map, potential, projectors, strengths, proj_atom, proj_chan):
    group = lax.axis_size("ga")
    grid_len = potential.shape[0]
    planes = grid_len // group
    fits = (
        planes == 4 * TRIPLE
        and 4 * grid_len % 128 == 0
        and coeffs.shape[1] == 1
        and coeffs.shape[2] % 256 == 0
        and 2 * projectors.shape[1] == 128
    )
    chosen = kernel_body if fits else plain_body
    return chosen(coeffs, cell_map, potential, projectors, strengths, proj_atom, proj_chan)


def solution(mesh):
    placed = (
        P(None, "band", "ga"),
        P("ga"),
        P(None, "ga", None),
        P(None, None, "ga"),
        P(),
        P(),
        P(),
    )
    return jax.shard_map(
        body,
        mesh=mesh,
        in_specs=placed,
        out_specs=(
            P(None, "band", "ga"),
            P("band"),
            P("band"),
            P(None, "band", None),
            P(None, "band", None),
        ),
        check_vma=False,
    )
```

```python
import functools

import jax
import jax.numpy as jnp
import numpy as np
from jax import lax
from jax.experimental import pallas as pl
from jax.experimental.pallas import tpu as pltpu
from jax.sharding import PartitionSpec as P

top_precision = lax.Precision.HIGHEST
kin_unit = 0.02
small_eps = 1e-06


def signed_freq(index_arr, grid_len):
    return jnp.where(index_arr < grid_len // 2, index_arr, index_arr - grid_len)


def wave_tables(grid_len, row_freq, col_freq, sign_val, factor):
    phase = row_freq[:, None] * col_freq[None, :] % grid_len
    angle = 2.0 * jnp.pi / grid_len * phase.astype(jnp.float32)
    return (jnp.cos(angle) * factor, jnp.sin(angle) * (sign_val * factor))


def block_table(cos_table, sin_table):
    upper = jnp.concatenate([cos_table, sin_table], axis=1)
    lower = jnp.concatenate([-sin_table, cos_table], axis=1)
    return jnp.concatenate([upper, lower], axis=0)


def quarter_turn(grid_vals):
    half_len = grid_vals.shape[-1] // 2
    return jnp.concatenate([-grid_vals[..., half_len:], grid_vals[..., :half_len]], axis=-1)


def mix_dim(grid_vals, cos_table, sin_table, pattern):
    direct = jnp.einsum(pattern, cos_table, grid_vals, precision=top_precision)
    turned = jnp.einsum(pattern, sin_table, quarter_turn(grid_vals), precision=top_precision)
    return direct + turned


def mix_last(grid_vals, table_full):
    row_width = grid_vals.shape[-1]
    product = jnp.dot(
        grid_vals.reshape(-1, row_width),
        table_full,
        precision=top_precision,
        preferred_element_type=jnp.float32,
    )
    return product.reshape(grid_vals.shape)


def band_dot(left_vec, right_vec, weight):
    return jnp.sum(left_vec * right_vec * weight, axis=(0, 2))


def per_band(values):
    return values[None, :, None]


def pair_products(left_vec, right_vec):

    def contract(first_part, second_part):
        return jnp.einsum("bg,cg->bc", first_part, second_part, precision=top_precision)

    real_part = contract(left_vec[0], right_vec[0]) + contract(left_vec[1], right_vec[1])
    imag_part = contract(left_vec[0], right_vec[1]) - contract(left_vec[1], right_vec[0])
    return jnp.stack([real_part, imag_part])


def precondition(residual, kinetic, kin_level):
    x_ratio = kinetic[None, :] / (1.5 * kin_level[:, None] + 1.0)
    numer_poly = 27.0 + x_ratio * (18.0 + x_ratio * (12.0 + 8.0 * x_ratio))
    square = x_ratio * x_ratio
    return residual * (numer_poly / (numer_poly + 16.0 * square * square))[None]


def coupling_matrix(proj_atom, proj_chan, strengths):
    atom_count = strengths.shape[0]
    chan_count = strengths.shape[1]
    symmetric = 0.5 * (strengths + jnp.swapaxes(strengths, 1, 2))
    atom_hot = (proj_atom[:, None] == jnp.arange(atom_count, dtype=jnp.int32)[None, :]).astype(
        jnp.float32
    )
    chan_hot = (proj_chan[:, None] == jnp.arange(chan_count, dtype=jnp.int32)[None, :]).astype(
        jnp.float32
    )
    rows_d = jnp.einsum("pa,pc,acd->pd", atom_hot, chan_hot, symmetric, precision=top_precision)
    same_atom = jnp.dot(
        atom_hot, atom_hot.T, precision=top_precision, preferred_element_type=jnp.float32
    )
    return same_atom * jnp.dot(
        rows_d, chan_hot.T, precision=top_precision, preferred_element_type=jnp.float32
    )


def combine(term_list):
    merged = {}
    for scalar, coef_map in term_list:
        for index_one, coef_a in coef_map.items():
            merged[index_one] = merged.get(index_one, 0.0) + scalar * coef_a
    return merged


def gram_form(gram_table, left_map, right_map, use_kin):
    running = 0.0
    for index_one, coef_a in left_map.items():
        for index_two, coef_b in right_map.items():
            running = running + coef_a * coef_b * gram_table[use_kin, index_one, index_two]
    return running


def new_pairs(first_new, last_new, kinds):
    pair_list = []
    for use_kin in kinds:
        for index_two in range(first_new, last_new):
            for index_one in range(index_two + 1):
                pair_list.append((index_one, index_two, use_kin))
    return pair_list


def plain_body(coeffs, cell_map, potential, projectors, strengths, proj_atom, proj_chan):
    ga_count = lax.axis_size("ga")
    grid_len = potential.shape[0]
    planes = grid_len // ga_count
    band_local = coeffs.shape[1]
    total_pw = coeffs.shape[2] * ga_count
    device = lax.axis_index("ga")
    plane_num = cell_map // (grid_len * grid_len)
    y_index = cell_map // grid_len % grid_len
    z_index = cell_map % grid_len
    freq_x = signed_freq(device + ga_count * plane_num, grid_len)
    freq_y = signed_freq(y_index, grid_len)
    freq_z = signed_freq(z_index, grid_len)
    kinetic = kin_unit * (freq_x * freq_x + freq_y * freq_y + freq_z * freq_z).astype(jnp.float32)
    kin_weight = kinetic[None, None, :]
    slot_re = (plane_num * grid_len + y_index) * (2 * grid_len) + z_index
    slot_im = slot_re + grid_len
    cell_count = planes * grid_len * 2 * grid_len
    natural = jnp.arange(grid_len, dtype=jnp.int32)
    cyclic = natural % planes * ga_count + natural // planes
    cos_fwd, sin_fwd = wave_tables(grid_len, natural, natural, 1.0, 1.0)
    cos_back, sin_back = wave_tables(grid_len, natural, natural, -1.0, 1.0 / grid_len)
    z_forward = block_table(cos_fwd, sin_fwd)
    z_backward = block_table(cos_back, sin_back)
    xcos_fwd, xsin_fwd = wave_tables(grid_len, natural, cyclic, 1.0, 1.0)
    xcos_back, xsin_back = wave_tables(grid_len, cyclic, natural, -1.0, 1.0 / grid_len)
    doubled = jnp.concatenate([potential, potential], axis=-1)
    coupling = coupling_matrix(proj_atom, proj_chan, strengths)

    def real_space(grid_vals):
        grid_vals = mix_dim(grid_vals, xcos_fwd, xsin_fwd, "kj,bjyw->bkyw")
        grid_vals = grid_vals * doubled[None]
        grid_vals = mix_dim(grid_vals, xcos_back, xsin_back, "jk,bkyw->bjyw")
        return lax.all_to_all(grid_vals, "ga", split_axis=1, concat_axis=2, tiled=True)

    def local_part(vectors):
        item_count = vectors.shape[1]
        flat_grid = jnp.zeros((item_count, cell_count), jnp.float32)
        flat_grid = flat_grid.at[:, slot_re].set(vectors[0]).at[:, slot_im].set(vectors[1])
        grid_vals = mix_last(
            flat_grid.reshape(item_count, planes, grid_len, 2 * grid_len), z_forward
        )
        grid_vals = mix_dim(grid_vals, cos_fwd, sin_fwd, "ky,bpyw->bpkw")
        grid_vals = real_space(
            lax.all_to_all(grid_vals, "ga", split_axis=2, concat_axis=1, tiled=True)
        )
        grid_vals = mix_dim(grid_vals, cos_back, sin_back, "ky,bpyw->bpkw")
        flat_grid = mix_last(grid_vals, z_backward).reshape(item_count, cell_count)
        return jnp.stack([flat_grid[:, slot_re], flat_grid[:, slot_im]])

    def contract(first_part, second_part):
        return jnp.einsum("pg,bg->pb", first_part, second_part, precision=top_precision)

    def spread(weights, proj_table):
        return jnp.einsum("pb,pg->bg", weights, proj_table, precision=top_precision)

    def projected_part(vectors):
        proj_re = contract(projectors[0], vectors[0]) + contract(projectors[1], vectors[1])
        proj_im = contract(projectors[0], vectors[1]) - contract(projectors[1], vectors[0])
        proj_re, proj_im = lax.psum((proj_re, proj_im), "ga")
        mixed_re = jnp.dot(
            coupling,
            proj_re / total_pw,
            precision=top_precision,
            preferred_element_type=jnp.float32,
        )
        mixed_im = jnp.dot(
            coupling,
            proj_im / total_pw,
            precision=top_precision,
            preferred_element_type=jnp.float32,
        )
        out_re = spread(mixed_re, projectors[0]) - spread(mixed_im, projectors[1])
        out_im = spread(mixed_re, projectors[1]) + spread(mixed_im, projectors[0])
        return jnp.stack([out_re, out_im])

    def apply_h(vectors):
        return kin_weight * vectors + local_part(vectors) + projected_part(vectors)

    def gram_sums(basis, pair_list):
        stacked = []
        for index_one, index_two, use_kin in pair_list:
            stacked.append(
                band_dot(basis[index_one], basis[index_two], kin_weight if use_kin else 1.0)
            )
        summed = lax.psum(jnp.stack(stacked), "ga") / total_pw
        found = {}
        for slot_num, entry in enumerate(pair_list):
            index_one, index_two, use_kin = entry
            found[use_kin, index_one, index_two] = summed[slot_num]
            found[use_kin, index_two, index_one] = summed[slot_num]
        return found

    def realize(coef_map, basis):
        running = jnp.zeros_like(basis[0])
        for index_one, coef_a in coef_map.items():
            running = (
                running
                + per_band(jnp.zeros((band_local,), jnp.float32) + coef_a) * basis[index_one]
            )
        return running

    h_zero = apply_h(coeffs)
    basis = [coeffs, h_zero]
    gram_table = gram_sums(basis, new_pairs(0, 2, (False, True)))
    psi_map = {0: 1.0}
    ham_map = {1: 1.0}
    eps_zero = gram_form(gram_table, psi_map, ham_map, False) / (
        gram_form(gram_table, psi_map, psi_map, False) + small_eps
    )
    r_map = combine([(1.0, ham_map), (-eps_zero, psi_map)])
    level_zero = gram_form(gram_table, r_map, r_map, True) / (
        gram_form(gram_table, r_map, r_map, False) + small_eps
    )
    p_zero = precondition(realize(r_map, basis), kinetic, level_zero)
    g_zero = apply_h(p_zero)
    basis = [coeffs, h_zero, p_zero, g_zero]
    gram_table.update(gram_sums(basis, new_pairs(2, 4, (False, True))))
    q_map = combine([(1.0, {3: 1.0}), (-eps_zero, {2: 1.0})])
    lam_zero = -gram_form(gram_table, r_map, q_map, False) / (
        gram_form(gram_table, q_map, q_map, False) + small_eps
    )
    psi_one_map = combine([(1.0, psi_map), (lam_zero, {2: 1.0})])
    h_one_map = combine([(1.0, ham_map), (lam_zero, {3: 1.0})])
    eps_one = gram_form(gram_table, psi_one_map, h_one_map, False) / (
        gram_form(gram_table, psi_one_map, psi_one_map, False) + small_eps
    )
    r_one_map = combine([(1.0, h_one_map), (-eps_one, psi_one_map)])
    change_map = combine([(1.0, r_map), (-1.0, r_one_map)])
    weight_one = gram_form(gram_table, r_map, change_map, False) / (
        gram_form(gram_table, change_map, change_map, False) + small_eps
    )
    step_mid = weight_one * lam_zero
    psi_mid_map = combine([(1.0, psi_map), (step_mid, {2: 1.0})])
    h_mid_map = combine([(1.0, ham_map), (step_mid, {3: 1.0})])
    r_mid_map = combine([(1.0, r_map), (-weight_one, change_map)])
    eps_mid = gram_form(gram_table, psi_mid_map, h_mid_map, False) / (
        gram_form(gram_table, psi_mid_map, psi_mid_map, False) + small_eps
    )
    level_mid = gram_form(gram_table, r_mid_map, r_mid_map, True) / (
        gram_form(gram_table, r_mid_map, r_mid_map, False) + small_eps
    )
    p_one = precondition(realize(r_mid_map, basis), kinetic, level_mid)
    g_one = apply_h(p_one)
    basis = [coeffs, h_zero, p_zero, g_zero, p_one, g_one]
    gram_table.update(gram_sums(basis, new_pairs(4, 6, (False,))))
    q_one_map = combine([(1.0, {5: 1.0}), (-eps_mid, {4: 1.0})])
    lam_one = -gram_form(gram_table, r_mid_map, q_one_map, False) / (
        gram_form(gram_table, q_one_map, q_one_map, False) + small_eps
    )
    new_map = combine([(1.0, psi_mid_map), (lam_one, {4: 1.0})])
    ham_new_map = combine([(1.0, h_mid_map), (lam_one, {5: 1.0})])
    norm_new = gram_form(gram_table, new_map, new_map, False) + small_eps
    energy = gram_form(gram_table, new_map, ham_new_map, False) / norm_new
    resid_map = combine([(1.0, ham_new_map), (-energy, new_map)])
    residual_norm = gram_form(gram_table, resid_map, resid_map, False) / norm_new
    new_bands = realize(new_map, basis)
    new_ham = realize(ham_new_map, basis)
    blank_rows = jnp.zeros((2, band_local, band_local * lax.axis_size("band")), jnp.float32)
    first_row = jnp.int32(0)
    over_rows = blank_rows
    ham_rows = blank_rows
    piece_bands = lax.all_gather(new_bands, "band", axis=1, tiled=True)
    piece_ham = lax.all_gather(new_ham, "band", axis=1, tiled=True)
    over_rows = lax.dynamic_update_slice_in_dim(
        over_rows, pair_products(new_bands, piece_bands), first_row, 2
    )
    ham_rows = lax.dynamic_update_slice_in_dim(
        ham_rows, pair_products(new_bands, piece_ham), first_row, 2
    )
    over_rows, ham_rows = (over_rows, ham_rows)
    over_rows, ham_rows = lax.psum((over_rows, ham_rows), "ga")
    correlation = over_rows / total_pw
    subspace = ham_rows / total_pw
    return (new_bands, energy, residual_norm, correlation, subspace)


QUAD = 4
TRIPLE = 3
MESH = pl.DeviceIdType.MESH


def split_const(values):
    high = np.asarray(values, np.float32).astype(jnp.bfloat16)
    low = (values - high.astype(np.float64)).astype(np.float32).astype(jnp.bfloat16)
    return np.stack([high, low])


def const_tables(grid_len, group):
    planes = grid_len // group
    chunks = planes // QUAD
    unit = 2.0 * np.pi / grid_len
    quarter = grid_len / 4.0
    chunk = np.arange(chunks)[:, None, None, None]
    dev = np.arange(group)[None, :, None, None]
    part = np.arange(2)[None, None, :, None]
    inner = np.arange(QUAD)[None, None, None, :]
    y_real = (dev * planes + chunk * QUAD + inner + 0 * part).reshape(-1)
    part_row = (part + 0 * (dev + chunk + inner)).reshape(-1)
    freq = np.arange(grid_len)
    phase = (y_real[:, None] * freq[None, :]) % grid_len
    tab_a = np.cos(unit * (phase - quarter * part_row[:, None]))
    tab_b = np.cos(unit * (phase + quarter * (1 - part_row[:, None])))
    wave = split_const(np.concatenate([tab_a, tab_b], axis=0))
    four = np.repeat(np.arange(4), grid_len)
    zed = np.tile(freq, 4)
    theta = 2.0 * np.pi * ((four[:, None] * four[None, :] % 4) / 4.0
                           + (zed[:, None] * zed[None, :] % grid_len) / grid_len)
    fourz = split_const(np.concatenate([np.cos(theta), np.sin(theta)], axis=1))
    dft = 2.0 * np.pi * np.outer(np.arange(group), np.arange(group)) / group
    real_mix = np.zeros((group, 2, QUAD, group, 2, QUAD))
    for row in range(QUAD):
        real_mix[:, 0, row, :, 0, row] = np.cos(dft)
        real_mix[:, 1, row, :, 1, row] = np.cos(dft)
        real_mix[:, 0, row, :, 1, row] = -np.sin(dft)
        real_mix[:, 1, row, :, 0, row] = np.sin(dft)
    size = group * 2 * QUAD
    real_mix = real_mix.reshape(size, size)

    def stacked(mat):
        high, low = split_const(mat)
        return np.concatenate([high, high, low], axis=1)

    across = np.stack([stacked(real_mix), stacked(real_mix.T)])
    b_lane = np.repeat(np.arange(TRIPLE), 4 * grid_len)
    a_lane = np.tile(np.repeat(np.arange(4), grid_len), TRIPLE)
    one = 2.0 * np.pi * (a_lane * b_lane) / planes
    two = unit * np.outer(np.arange(group), TRIPLE * a_lane + b_lane)
    lane_tw = np.stack([np.cos(one), np.sin(one)]).astype(np.float32)[:, None, :]
    dev_tw = np.stack([np.cos(two), np.sin(two)]).astype(np.float32)[:, :, None, :]
    return wave, fourz, across, lane_tw, dev_tw


def two_parts(values):
    high = values.astype(jnp.bfloat16)
    low = (values - high.astype(jnp.float32)).astype(jnp.bfloat16)
    return high, low


def bdot(left, right):
    return jnp.dot(left, right, preferred_element_type=jnp.float32)


def sweep_kernel(
    dims,
    coeffs_ref, cell_ref, potential_ref, proj_ref, strength_ref, atom_ref, chan_ref,
    wave_ref, fourz_ref, across_ref, lane_ref, dev_ref,
    new_ref, scal_ref,
    hot_ref, hot_t_ref, ta_ref, tb_ref, key_ref, pot_ref,
    fsend, frecv, bsend, brecv, psend, precv, gsend, grecv, nsend, nrecv, csend, crecv,
    fs_sem, fr_sem, bs_sem, br_sem, ps_sem, pr_sem, gs_sem, gr_sem, ns_sem, nr_sem, cs_sem, cr_sem,
):
    group, bands, chunks, grid_len, total_pw, pw = dims
    rows = group * 2 * QUAD
    lanes = TRIPLE * 4 * grid_len
    quad_lanes = 4 * grid_len
    me = lax.axis_index("ga")
    band = lax.axis_index("band")

    barrier = pltpu.get_barrier_semaphore()
    for off in range(1, group):
        pl.semaphore_signal(barrier, inc=1, device_id={"ga": lax.rem(me + off, group)}, device_id_type=MESH)
    for off in range(1, bands):
        pl.semaphore_signal(barrier, inc=1, device_id={"band": lax.rem(band + off, bands)}, device_id_type=MESH)

    def whole(values):
        return jnp.floor(values)

    cell = cell_ref[...].astype(jnp.float32)
    plane = whole((cell + 0.5) * (1.0 / (grid_len * grid_len)))
    in_plane = cell - plane * (grid_len * grid_len)
    y_num = whole((in_plane + 0.5) * (1.0 / grid_len))
    z_num = in_plane - y_num * grid_len
    key_ref[...] = plane * grid_len + z_num

    def signed(values):
        return jnp.where(2.0 * values < grid_len, values, values - grid_len)

    f_x = signed(plane * group + me.astype(jnp.float32))
    f_y, f_z = signed(y_num), signed(z_num)
    kin = kin_unit * (f_x * f_x + f_y * f_y + f_z * f_z)

    def build_hot(step, carry):
        at = pl.multiple_of(step * 128, 128)
        key_col = jnp.transpose(jnp.broadcast_to(key_ref[:, pl.ds(at, 128)], (128, 128)))
        lane_id = lax.broadcasted_iota(jnp.int32, (128, 128), 1).astype(jnp.float32)
        for k in range(lanes // 128):
            hit = jnp.where(lane_id == key_col - 128.0 * k, 1.0, 0.0)
            hot_ref[pl.ds(at, 128), k * 128:(k + 1) * 128] = hit.astype(jnp.bfloat16)
        return carry

    lax.fori_loop(0, pw // 128, build_hot, 0)
    y_hot = jnp.where(lax.broadcasted_iota(jnp.int32, (grid_len, pw), 0).astype(jnp.float32) == y_num, 1.0, 0.0).astype(jnp.bfloat16)
    for part in range(chunks):
        for table, base in ((ta_ref, 0), (tb_ref, chunks * rows)):
            at = base + part * rows
            table[part] = bdot(wave_ref[0, at:at + rows, :], y_hot) + bdot(wave_ref[1, at:at + rows, :], y_hot)

    def build_turn():
        turn_rows = 128

        def step_turn(step, carry):
            at = pl.multiple_of(step * turn_rows, turn_rows)
            row_id = (lax.broadcasted_iota(jnp.int32, (turn_rows, pw), 0) + at).astype(jnp.float32)
            hot_t_ref[pl.ds(at, turn_rows), :] = jnp.where(row_id == key_ref[...], 1.0, 0.0).astype(jnp.bfloat16)
            return carry

        lax.fori_loop(0, lanes // turn_rows, step_turn, 0)

    def build_potential():
        for part in range(chunks):
            for b in range(TRIPLE):
                for a in range(4):
                    at = (b * 4 + a) * grid_len
                    block = potential_ref[:, TRIPLE * a + b, part * QUAD:(part + 1) * QUAD, :] * (1.0 / grid_len**3)
                    pot_ref[part, :, :QUAD, at:at + grid_len] = block
                    pot_ref[part, :, QUAD:, at:at + grid_len] = block

    def build_coupling():
        atoms, chans = strength_ref.shape[0] // strength_ref.shape[1], strength_ref.shape[1]
        size = atoms * chans
        ident = atom_ref[...] * chans + chan_ref[...]
        hot = (lax.broadcasted_iota(jnp.int32, (size, ident.shape[1]), 0) == ident).astype(jnp.float32)
        row_at = lax.broadcasted_iota(jnp.int32, (size, size), 0)
        col_at = lax.broadcasted_iota(jnp.int32, (size, size), 1)
        tiled = jnp.concatenate([strength_ref[...]] * atoms, axis=1)
        same = (row_at // chans == col_at // chans).astype(jnp.float32)
        block = tiled * same
        block = 0.5 * (block + jnp.transpose(block))
        half = lax.dot_general(hot, block, (((0,), (0,)), ((), ())), precision=top_precision, preferred_element_type=jnp.float32)
        return jnp.dot(half, hot, precision=top_precision, preferred_element_type=jnp.float32)

    pl.semaphore_wait(barrier, group + bands - 2)

    sign = jnp.where(lax.broadcasted_iota(jnp.int32, (1, 2 * QUAD, 1), 1) < QUAD, -1.0, 1.0).astype(jnp.float32)

    def times_i(values):
        return pltpu.roll(values, QUAD, 1) * sign

    def lane_split(values):
        return [values[..., k * quad_lanes:(k + 1) * quad_lanes] for k in range(TRIPLE)]

    def mix_fourz(triple, direction):
        stacked = jnp.concatenate([t.reshape(rows, quad_lanes) for t in triple], axis=0)
        high, low = two_parts(stacked)
        out = bdot(high, fourz_ref[0]) + bdot(low, fourz_ref[0]) + bdot(high, fourz_ref[1])
        out = out.reshape(TRIPLE * group, 2 * QUAD, 2 * quad_lanes)
        mixed = out[..., :quad_lanes] + direction * times_i(out[..., quad_lanes:])
        return [mixed[k * group:(k + 1) * group] for k in range(TRIPLE)]

    def turn_lane(triple, direction):
        done = [triple[0]]
        for k in range(1, TRIPLE):
            at = slice(k * quad_lanes, (k + 1) * quad_lanes)
            done.append(triple[k] * lane_ref[0, :, at][None] + direction * times_i(triple[k]) * lane_ref[1, :, at][None])
        return done

    def three(triple, direction):
        total = triple[1] + triple[2]
        diff = times_i(triple[1] - triple[2]) * (direction * 0.8660254037844386)
        base = triple[0] - 0.5 * total
        return [triple[0] + total, base + diff, base - diff]

    def turn_dev(values, direction):
        return values * dev_ref[0] + direction * times_i(values) * dev_ref[1]

    def mix_devices(values, which):
        high, low = two_parts(values.reshape(rows, lanes))
        return bdot(across_ref[which], jnp.concatenate([high, low, high], axis=0))

    def all_sum(local, send, recv, send_sem, recv_sem, shape_at):
        send[shape_at] = local
        recv[shape_at, me] = local
        for off in range(1, group):
            pltpu.make_async_remote_copy(
                src_ref=send.at[shape_at], dst_ref=recv.at[shape_at, me],
                send_sem=send_sem.at[shape_at, off - 1], recv_sem=recv_sem.at[shape_at, off - 1],
                device_id={"ga": lax.rem(me + off, group)}, device_id_type=MESH).start()

    def all_sum_end(send, recv, send_sem, recv_sem, shape_at):
        for off in range(1, group):
            pltpu.make_async_remote_copy(
                src_ref=send.at[shape_at], dst_ref=recv.at[shape_at, lax.rem(me + group - off, group)],
                send_sem=send_sem.at[shape_at, off - 1], recv_sem=recv_sem.at[shape_at, off - 1],
                device_id={"ga": lax.rem(me + off, group)}, device_id_type=MESH).wait()
        running = recv[shape_at, 0]
        for dev in range(1, group):
            running = running + recv[shape_at, dev]
        return running

    def piece(turn, part, off, send, recv, send_sem, recv_sem, incoming):
        peer = lax.rem(me + off, group)
        source = lax.rem(me + group - off, group) if incoming else me
        return pltpu.make_async_remote_copy(
            src_ref=send.at[turn, part, peer], dst_ref=recv.at[turn, part, source],
            send_sem=send_sem.at[turn, part, off - 1], recv_sem=recv_sem.at[turn, part, off - 1],
            device_id={"ga": peer}, device_id_type=MESH)

    def apply_h(turn, vector):
        v_re, v_im = vector[0:1], vector[1:2]
        fwd = (fsend, frecv, fs_sem, fr_sem)
        back = (bsend, brecv, bs_sem, br_sem)

        def put(part, carry):
            high, low = two_parts(ta_ref[part] * v_re + tb_ref[part] * v_im)
            out = bdot(jnp.concatenate([high, low], axis=0), hot_ref[...])
            out = (out[:rows] + out[rows:]).reshape(group, 2 * QUAD, lanes)
            fsend[turn, part] = out
            frecv[turn, part, me] = fsend[turn, part, me]
            for off in range(1, group):
                piece(turn, part, off, *fwd, False).start()
            return carry

        lax.fori_loop(0, chunks, put, 0)
        sums = lax.dot_general(vector, proj_ref[...], (((1,), (1,)), ((), ())), precision=top_precision, preferred_element_type=jnp.float32)
        all_sum(sums, psend, precv, ps_sem, pr_sem, turn)
        if turn == 0:
            build_potential()
            shared.append(build_coupling())
            build_turn()

        def middle(part, carry):
            for off in range(1, group):
                piece(turn, part, off, *fwd, True).wait()
            triple = turn_lane(three(lane_split(frecv[turn, part]), 1.0), 1.0)
            values = turn_dev(jnp.concatenate(mix_fourz(triple, 1.0), axis=-1), 1.0)
            values = mix_devices(values, 0) * pot_ref[part].reshape(rows, lanes)
            values = mix_devices(values, 1).reshape(group, 2 * QUAD, lanes)
            triple = mix_fourz(lane_split(turn_dev(values, -1.0)), -1.0)
            triple = three(turn_lane(triple, -1.0), -1.0)
            bsend[turn, part] = jnp.concatenate(triple, axis=-1)
            brecv[turn, part, me] = bsend[turn, part, me]
            for off in range(1, group):
                piece(turn, part, off, *back, False).start()
            return carry

        lax.fori_loop(0, chunks, middle, 0)
        sums = all_sum_end(psend, precv, ps_sem, pr_sem, turn) * (1.0 / total_pw)
        half = sums.shape[1] // 2
        pair = jnp.concatenate([
            sums[0:1, :half] + sums[1:2, half:], sums[1:2, :half] - sums[0:1, half:]], axis=0)
        mixed = jnp.dot(pair, shared[0], precision=top_precision, preferred_element_type=jnp.float32)
        m_re, m_im = mixed[0:1], mixed[1:2]
        weights = jnp.concatenate([
            jnp.concatenate([m_re, -m_im], axis=1), jnp.concatenate([m_im, m_re], axis=1)], axis=0)
        nonlocal_part = jnp.dot(weights, proj_ref[...], precision=top_precision, preferred_element_type=jnp.float32)
        start = kin * vector + nonlocal_part

        def take(part, carry):
            run_re, run_im = carry
            for off in range(1, group):
                piece(turn, part, off, *back, True).wait()
            high, low = two_parts(brecv[turn, part].reshape(rows, lanes))
            out = bdot(jnp.concatenate([high, low], axis=0), hot_t_ref[...])
            out = out[:rows] + out[rows:]
            run_re = run_re + jnp.sum(ta_ref[part] * out, axis=0, keepdims=True)
            run_im = run_im + jnp.sum(tb_ref[part] * out, axis=0, keepdims=True)
            return run_re, run_im

        run_re, run_im = lax.fori_loop(0, chunks, take, (start[0:1], start[1:2]))
        return jnp.concatenate([run_re, run_im], axis=0)

    def as_row(values):
        total = jnp.sum(jnp.sum(values, axis=0, keepdims=True), axis=1, keepdims=True)
        return jnp.broadcast_to(total, (1, 128))

    row_count = gsend.shape[1]

    def gram_sums(turn, basis, pair_list):
        found_rows = []
        for one, two, use_kin in pair_list:
            product = basis[one] * basis[two]
            found_rows.append(as_row(product * kin if use_kin else product))
        found_rows += [jnp.zeros((1, 128), jnp.float32)] * (row_count - len(found_rows))
        all_sum(jnp.concatenate(found_rows, axis=0), gsend, grecv, gs_sem, gr_sem, turn)
        summed = all_sum_end(gsend, grecv, gs_sem, gr_sem, turn) * (1.0 / total_pw)
        found = {}
        for slot, (one, two, use_kin) in enumerate(pair_list):
            value = summed[slot:slot + 1]
            found[use_kin, one, two] = value
            found[use_kin, two, one] = value
        return found

    def realize(coef_map, basis):
        running = 0.0
        for index, coef in coef_map.items():
            running = running + (basis[index] if isinstance(coef, float) and coef == 1.0 else spread_row(coef) * basis[index])
        return running

    def spread_row(coef):
        return coef if isinstance(coef, float) else coef[:, 0:1]

    def smooth(residual, level):
        ratio = kin / (1.5 * level[:, 0:1] + 1.0)
        poly = 27.0 + ratio * (18.0 + ratio * (12.0 + 8.0 * ratio))
        square = ratio * ratio
        return residual * (poly / (poly + 16.0 * square * square))

    shared = []
    coeffs = coeffs_ref[:, 0, :]
    h_zero = apply_h(0, coeffs)
    basis = [coeffs, h_zero]
    gram = gram_sums(0, basis, new_pairs(0, 2, (False, True)))
    psi = {0: 1.0}
    ham = {1: 1.0}
    eps_zero = gram_form(gram, psi, ham, False) / (gram_form(gram, psi, psi, False) + small_eps)
    r_map = combine([(1.0, ham), (-eps_zero, psi)])
    level = gram_form(gram, r_map, r_map, True) / (gram_form(gram, r_map, r_map, False) + small_eps)
    p_zero = smooth(realize(r_map, basis), level)
    g_zero = apply_h(1, p_zero)
    basis += [p_zero, g_zero]
    gram.update(gram_sums(1, basis, new_pairs(2, 4, (False, True))))
    q_map = combine([(1.0, {3: 1.0}), (-eps_zero, {2: 1.0})])
    lam_zero = -gram_form(gram, r_map, q_map, False) / (gram_form(gram, q_map, q_map, False) + small_eps)
    psi_one = combine([(1.0, psi), (lam_zero, {2: 1.0})])
    h_one = combine([(1.0, ham), (lam_zero, {3: 1.0})])
    eps_one = gram_form(gram, psi_one, h_one, False) / (gram_form(gram, psi_one, psi_one, False) + small_eps)
    r_one = combine([(1.0, h_one), (-eps_one, psi_one)])
    change = combine([(1.0, r_map), (-1.0, r_one)])
    weight = gram_form(gram, r_map, change, False) / (gram_form(gram, change, change, False) + small_eps)
    step = weight * lam_zero
    psi_mid = combine([(1.0, psi), (step, {2: 1.0})])
    h_mid = combine([(1.0, ham), (step, {3: 1.0})])
    r_mid = combine([(1.0, r_map), (-weight, change)])
    eps_mid = gram_form(gram, psi_mid, h_mid, False) / (gram_form(gram, psi_mid, psi_mid, False) + small_eps)
    level = gram_form(gram, r_mid, r_mid, True) / (gram_form(gram, r_mid, r_mid, False) + small_eps)
    p_one = smooth(realize(r_mid, basis), level)
    g_one = apply_h(2, p_one)
    basis += [p_one, g_one]
    gram.update(gram_sums(2, basis, new_pairs(4, 6, (False,))))
    q_one = combine([(1.0, {5: 1.0}), (-eps_mid, {4: 1.0})])
    lam_one = -gram_form(gram, r_mid, q_one, False) / (gram_form(gram, q_one, q_one, False) + small_eps)
    new_map = combine([(1.0, psi_mid), (lam_one, {4: 1.0})])
    ham_new = combine([(1.0, h_mid), (lam_one, {5: 1.0})])
    norm_new = gram_form(gram, new_map, new_map, False) + small_eps
    energy = gram_form(gram, new_map, ham_new, False) / norm_new
    resid = combine([(1.0, ham_new), (-energy, new_map)])
    resid_norm = gram_form(gram, resid, resid, False) / norm_new
    new = realize(new_map, basis)
    new_h = realize(ham_new, basis)
    new_ref[...] = new
    both = jnp.concatenate([new, new_h, jnp.zeros((4, pw), jnp.float32)], axis=0)
    nsend[...] = both
    nrecv[band] = both

    def swap(off, incoming):
        source = lax.rem(band + bands - off, bands) if incoming else band
        return pltpu.make_async_remote_copy(
            src_ref=nsend, dst_ref=nrecv.at[source], send_sem=ns_sem.at[off - 1], recv_sem=nr_sem.at[off - 1],
            device_id={"band": lax.rem(band + off, bands)}, device_id_type=MESH)

    for off in range(1, bands):
        swap(off, False).start()
    for off in range(1, bands):
        swap(off, True).wait()
    found_rows = []
    for first in (0, 2):
        for imag in (False, True):
            for other in range(bands):
                o_re = nrecv[other, first:first + 1]
                o_im = nrecv[other, first + 1:first + 2]
                if imag:
                    found_rows.append(as_row(new[0:1] * o_im - new[1:2] * o_re))
                else:
                    found_rows.append(as_row(new[0:1] * o_re + new[1:2] * o_im))
    all_sum(jnp.concatenate(found_rows, axis=0), csend, crecv, cs_sem, cr_sem, 0)
    summed = all_sum_end(csend, crecv, cs_sem, cr_sem, 0) * (1.0 / total_pw)
    scal_ref[...] = jnp.concatenate([summed, energy, resid_norm, jnp.zeros((6, 128), jnp.float32)], axis=0)


def finish_kernel(bands, new_ref, scal_ref, bands_ref, energy_ref, norm_ref, corr_ref, sub_ref):
    bands_ref[:, 0, :] = new_ref[...]
    lane = lax.broadcasted_iota(jnp.int32, (1, bands), 1)
    for ref, base in ((corr_ref, 0), (sub_ref, 2 * bands)):
        for part in range(2):
            row = jnp.zeros((1, bands), jnp.float32)
            for other in range(bands):
                at = base + part * bands + other
                row = jnp.where(lane == other, scal_ref[at:at + 1, :bands], row)
            ref[part] = row
    energy_ref[0] = scal_ref[4 * bands, 0]
    norm_ref[0] = scal_ref[4 * bands + 1, 0]


def kernel_body(coeffs, cell_map, potential, projectors, strengths, proj_atom, proj_chan):
    group = lax.axis_size("ga")
    bands = lax.axis_size("band")
    grid_len = potential.shape[0]
    planes = grid_len // group
    chunks = planes // QUAD
    pw = coeffs.shape[2]
    total_pw = pw * group
    rows = group * 2 * QUAD
    lanes = planes * grid_len
    proj_rows = 2 * projectors.shape[1]
    tables = [jnp.asarray(t) for t in const_tables(grid_len, group)]
    gram_rows = 16
    piece_shape = (3, chunks, group, 2 * QUAD, lanes)
    dma = pltpu.SemaphoreType.DMA
    vmem = pl.BlockSpec(memory_space=pltpu.VMEM)
    f32 = jnp.float32
    new, scal = pl.pallas_call(
        functools.partial(sweep_kernel, (group, bands, chunks, grid_len, total_pw, pw)),
        out_shape=(
            jax.ShapeDtypeStruct((2, pw), f32),
            jax.ShapeDtypeStruct((4 * bands + 8, 128), f32),
        ),
        in_specs=[vmem] * 12,
        out_specs=(vmem, vmem),
        scratch_shapes=[
            pltpu.VMEM((pw, lanes), jnp.bfloat16),
            pltpu.VMEM((lanes, pw), jnp.bfloat16),
            pltpu.VMEM((chunks, rows, pw), f32),
            pltpu.VMEM((chunks, rows, pw), f32),
            pltpu.VMEM((1, pw), f32),
            pltpu.VMEM((chunks, group, 2 * QUAD, lanes), f32),
            pltpu.VMEM(piece_shape, f32),
            pltpu.VMEM(piece_shape, f32),
            pltpu.VMEM(piece_shape, f32),
            pltpu.VMEM(piece_shape, f32),
            pltpu.VMEM((3, 2, proj_rows), f32),
            pltpu.VMEM((3, group, 2, proj_rows), f32),
            pltpu.VMEM((3, gram_rows, 128), f32),
            pltpu.VMEM((3, group, gram_rows, 128), f32),
            pltpu.VMEM((8, pw), f32),
            pltpu.VMEM((bands, 8, pw), f32),
            pltpu.VMEM((1, 4 * bands, 128), f32),
            pltpu.VMEM((1, group, 4 * bands, 128), f32),
            dma((3, chunks, group - 1)), dma((3, chunks, group - 1)),
            dma((3, chunks, group - 1)), dma((3, chunks, group - 1)),
            dma((3, group - 1)), dma((3, group - 1)),
            dma((3, group - 1)), dma((3, group - 1)),
            dma((bands - 1,)), dma((bands - 1,)),
            dma((1, group - 1)), dma((1, group - 1)),
        ],
        compiler_params=pltpu.CompilerParams(
            collective_id=0, has_side_effects=True, vmem_limit_bytes=60 * 1024 * 1024
        ),
        name="sweeps",
    )(
        coeffs, cell_map.reshape(1, pw), potential.reshape(group, planes, planes, grid_len),
        projectors.reshape(proj_rows, pw), strengths.reshape(-1, strengths.shape[2]),
        proj_atom.reshape(1, -1), proj_chan.reshape(1, -1), *tables,
    )

    smem = pl.BlockSpec(memory_space=pltpu.SMEM)
    return pl.pallas_call(
        functools.partial(finish_kernel, bands),
        out_shape=(
            jax.ShapeDtypeStruct((2, 1, pw), f32),
            jax.ShapeDtypeStruct((1,), f32),
            jax.ShapeDtypeStruct((1,), f32),
            jax.ShapeDtypeStruct((2, 1, bands), f32),
            jax.ShapeDtypeStruct((2, 1, bands), f32),
        ),
        in_specs=[vmem, vmem],
        out_specs=(vmem, smem, smem, vmem, vmem),
        name="finish",
    )(new, scal)


def body(coeffs, cell_map, potential, projectors, strengths, proj_atom, proj_chan):
    group = lax.axis_size("ga")
    grid_len = potential.shape[0]
    planes = grid_len // group
    fits = (
        planes == 4 * TRIPLE
        and 4 * grid_len % 128 == 0
        and coeffs.shape[1] == 1
        and coeffs.shape[2] % 256 == 0
        and 2 * projectors.shape[1] == 128
    )
    chosen = kernel_body if fits else plain_body
    return chosen(coeffs, cell_map, potential, projectors, strengths, proj_atom, proj_chan)


def solution(mesh):
    placed = (
        P(None, "band", "ga"),
        P("ga"),
        P(None, "ga", None),
        P(None, None, "ga"),
        P(),
        P(),
        P(),
    )
    return jax.shard_map(
        body,
        mesh=mesh,
        in_specs=placed,
        out_specs=(
            P(None, "band", "ga"),
            P("band"),
            P("band"),
            P(None, "band", None),
            P(None, "band", None),
        ),
        check_vma=False,
    )
```

```python
import functools

import jax
import jax.numpy as jnp
import numpy as np
from jax import lax
from jax.experimental import pallas as pl
from jax.experimental.pallas import tpu as pltpu
from jax.sharding import PartitionSpec as P

top_precision = lax.Precision.HIGHEST
kin_unit = 0.02
small_eps = 1e-06


def signed_freq(index_arr, grid_len):
    return jnp.where(index_arr < grid_len // 2, index_arr, index_arr - grid_len)


def wave_tables(grid_len, row_freq, col_freq, sign_val, factor):
    phase = row_freq[:, None] * col_freq[None, :] % grid_len
    angle = 2.0 * jnp.pi / grid_len * phase.astype(jnp.float32)
    return (jnp.cos(angle) * factor, jnp.sin(angle) * (sign_val * factor))


def block_table(cos_table, sin_table):
    upper = jnp.concatenate([cos_table, sin_table], axis=1)
    lower = jnp.concatenate([-sin_table, cos_table], axis=1)
    return jnp.concatenate([upper, lower], axis=0)


def quarter_turn(grid_vals):
    half_len = grid_vals.shape[-1] // 2
    return jnp.concatenate([-grid_vals[..., half_len:], grid_vals[..., :half_len]], axis=-1)


def mix_dim(grid_vals, cos_table, sin_table, pattern):
    direct = jnp.einsum(pattern, cos_table, grid_vals, precision=top_precision)
    turned = jnp.einsum(pattern, sin_table, quarter_turn(grid_vals), precision=top_precision)
    return direct + turned


def mix_last(grid_vals, table_full):
    row_width = grid_vals.shape[-1]
    product = jnp.dot(
        grid_vals.reshape(-1, row_width),
        table_full,
        precision=top_precision,
        preferred_element_type=jnp.float32,
    )
    return product.reshape(grid_vals.shape)


def band_dot(left_vec, right_vec, weight):
    return jnp.sum(left_vec * right_vec * weight, axis=(0, 2))


def per_band(values):
    return values[None, :, None]


def pair_products(left_vec, right_vec):

    def contract(first_part, second_part):
        return jnp.einsum("bg,cg->bc", first_part, second_part, precision=top_precision)

    real_part = contract(left_vec[0], right_vec[0]) + contract(left_vec[1], right_vec[1])
    imag_part = contract(left_vec[0], right_vec[1]) - contract(left_vec[1], right_vec[0])
    return jnp.stack([real_part, imag_part])


def precondition(residual, kinetic, kin_level):
    x_ratio = kinetic[None, :] / (1.5 * kin_level[:, None] + 1.0)
    numer_poly = 27.0 + x_ratio * (18.0 + x_ratio * (12.0 + 8.0 * x_ratio))
    square = x_ratio * x_ratio
    return residual * (numer_poly / (numer_poly + 16.0 * square * square))[None]


def coupling_matrix(proj_atom, proj_chan, strengths):
    atom_count = strengths.shape[0]
    chan_count = strengths.shape[1]
    symmetric = 0.5 * (strengths + jnp.swapaxes(strengths, 1, 2))
    atom_hot = (proj_atom[:, None] == jnp.arange(atom_count, dtype=jnp.int32)[None, :]).astype(
        jnp.float32
    )
    chan_hot = (proj_chan[:, None] == jnp.arange(chan_count, dtype=jnp.int32)[None, :]).astype(
        jnp.float32
    )
    rows_d = jnp.einsum("pa,pc,acd->pd", atom_hot, chan_hot, symmetric, precision=top_precision)
    same_atom = jnp.dot(
        atom_hot, atom_hot.T, precision=top_precision, preferred_element_type=jnp.float32
    )
    return same_atom * jnp.dot(
        rows_d, chan_hot.T, precision=top_precision, preferred_element_type=jnp.float32
    )


def combine(term_list):
    merged = {}
    for scalar, coef_map in term_list:
        for index_one, coef_a in coef_map.items():
            merged[index_one] = merged.get(index_one, 0.0) + scalar * coef_a
    return merged


def gram_form(gram_table, left_map, right_map, use_kin):
    running = 0.0
    for index_one, coef_a in left_map.items():
        for index_two, coef_b in right_map.items():
            running = running + coef_a * coef_b * gram_table[use_kin, index_one, index_two]
    return running


def new_pairs(first_new, last_new, kinds):
    pair_list = []
    for use_kin in kinds:
        for index_two in range(first_new, last_new):
            for index_one in range(index_two + 1):
                pair_list.append((index_one, index_two, use_kin))
    return pair_list


def plain_body(coeffs, cell_map, potential, projectors, strengths, proj_atom, proj_chan):
    ga_count = lax.axis_size("ga")
    grid_len = potential.shape[0]
    planes = grid_len // ga_count
    band_local = coeffs.shape[1]
    total_pw = coeffs.shape[2] * ga_count
    device = lax.axis_index("ga")
    plane_num = cell_map // (grid_len * grid_len)
    y_index = cell_map // grid_len % grid_len
    z_index = cell_map % grid_len
    freq_x = signed_freq(device + ga_count * plane_num, grid_len)
    freq_y = signed_freq(y_index, grid_len)
    freq_z = signed_freq(z_index, grid_len)
    kinetic = kin_unit * (freq_x * freq_x + freq_y * freq_y + freq_z * freq_z).astype(jnp.float32)
    kin_weight = kinetic[None, None, :]
    slot_re = (plane_num * grid_len + y_index) * (2 * grid_len) + z_index
    slot_im = slot_re + grid_len
    cell_count = planes * grid_len * 2 * grid_len
    natural = jnp.arange(grid_len, dtype=jnp.int32)
    cyclic = natural % planes * ga_count + natural // planes
    cos_fwd, sin_fwd = wave_tables(grid_len, natural, natural, 1.0, 1.0)
    cos_back, sin_back = wave_tables(grid_len, natural, natural, -1.0, 1.0 / grid_len)
    z_forward = block_table(cos_fwd, sin_fwd)
    z_backward = block_table(cos_back, sin_back)
    xcos_fwd, xsin_fwd = wave_tables(grid_len, natural, cyclic, 1.0, 1.0)
    xcos_back, xsin_back = wave_tables(grid_len, cyclic, natural, -1.0, 1.0 / grid_len)
    doubled = jnp.concatenate([potential, potential], axis=-1)
    coupling = coupling_matrix(proj_atom, proj_chan, strengths)

    def real_space(grid_vals):
        grid_vals = mix_dim(grid_vals, xcos_fwd, xsin_fwd, "kj,bjyw->bkyw")
        grid_vals = grid_vals * doubled[None]
        grid_vals = mix_dim(grid_vals, xcos_back, xsin_back, "jk,bkyw->bjyw")
        return lax.all_to_all(grid_vals, "ga", split_axis=1, concat_axis=2, tiled=True)

    def local_part(vectors):
        item_count = vectors.shape[1]
        flat_grid = jnp.zeros((item_count, cell_count), jnp.float32)
        flat_grid = flat_grid.at[:, slot_re].set(vectors[0]).at[:, slot_im].set(vectors[1])
        grid_vals = mix_last(
            flat_grid.reshape(item_count, planes, grid_len, 2 * grid_len), z_forward
        )
        grid_vals = mix_dim(grid_vals, cos_fwd, sin_fwd, "ky,bpyw->bpkw")
        grid_vals = real_space(
            lax.all_to_all(grid_vals, "ga", split_axis=2, concat_axis=1, tiled=True)
        )
        grid_vals = mix_dim(grid_vals, cos_back, sin_back, "ky,bpyw->bpkw")
        flat_grid = mix_last(grid_vals, z_backward).reshape(item_count, cell_count)
        return jnp.stack([flat_grid[:, slot_re], flat_grid[:, slot_im]])

    def contract(first_part, second_part):
        return jnp.einsum("pg,bg->pb", first_part, second_part, precision=top_precision)

    def spread(weights, proj_table):
        return jnp.einsum("pb,pg->bg", weights, proj_table, precision=top_precision)

    def projected_part(vectors):
        proj_re = contract(projectors[0], vectors[0]) + contract(projectors[1], vectors[1])
        proj_im = contract(projectors[0], vectors[1]) - contract(projectors[1], vectors[0])
        proj_re, proj_im = lax.psum((proj_re, proj_im), "ga")
        mixed_re = jnp.dot(
            coupling,
            proj_re / total_pw,
            precision=top_precision,
            preferred_element_type=jnp.float32,
        )
        mixed_im = jnp.dot(
            coupling,
            proj_im / total_pw,
            precision=top_precision,
            preferred_element_type=jnp.float32,
        )
        out_re = spread(mixed_re, projectors[0]) - spread(mixed_im, projectors[1])
        out_im = spread(mixed_re, projectors[1]) + spread(mixed_im, projectors[0])
        return jnp.stack([out_re, out_im])

    def apply_h(vectors):
        return kin_weight * vectors + local_part(vectors) + projected_part(vectors)

    def gram_sums(basis, pair_list):
        stacked = []
        for index_one, index_two, use_kin in pair_list:
            stacked.append(
                band_dot(basis[index_one], basis[index_two], kin_weight if use_kin else 1.0)
            )
        summed = lax.psum(jnp.stack(stacked), "ga") / total_pw
        found = {}
        for slot_num, entry in enumerate(pair_list):
            index_one, index_two, use_kin = entry
            found[use_kin, index_one, index_two] = summed[slot_num]
            found[use_kin, index_two, index_one] = summed[slot_num]
        return found

    def realize(coef_map, basis):
        running = jnp.zeros_like(basis[0])
        for index_one, coef_a in coef_map.items():
            running = (
                running
                + per_band(jnp.zeros((band_local,), jnp.float32) + coef_a) * basis[index_one]
            )
        return running

    h_zero = apply_h(coeffs)
    basis = [coeffs, h_zero]
    gram_table = gram_sums(basis, new_pairs(0, 2, (False, True)))
    psi_map = {0: 1.0}
    ham_map = {1: 1.0}
    eps_zero = gram_form(gram_table, psi_map, ham_map, False) / (
        gram_form(gram_table, psi_map, psi_map, False) + small_eps
    )
    r_map = combine([(1.0, ham_map), (-eps_zero, psi_map)])
    level_zero = gram_form(gram_table, r_map, r_map, True) / (
        gram_form(gram_table, r_map, r_map, False) + small_eps
    )
    p_zero = precondition(realize(r_map, basis), kinetic, level_zero)
    g_zero = apply_h(p_zero)
    basis = [coeffs, h_zero, p_zero, g_zero]
    gram_table.update(gram_sums(basis, new_pairs(2, 4, (False, True))))
    q_map = combine([(1.0, {3: 1.0}), (-eps_zero, {2: 1.0})])
    lam_zero = -gram_form(gram_table, r_map, q_map, False) / (
        gram_form(gram_table, q_map, q_map, False) + small_eps
    )
    psi_one_map = combine([(1.0, psi_map), (lam_zero, {2: 1.0})])
    h_one_map = combine([(1.0, ham_map), (lam_zero, {3: 1.0})])
    eps_one = gram_form(gram_table, psi_one_map, h_one_map, False) / (
        gram_form(gram_table, psi_one_map, psi_one_map, False) + small_eps
    )
    r_one_map = combine([(1.0, h_one_map), (-eps_one, psi_one_map)])
    change_map = combine([(1.0, r_map), (-1.0, r_one_map)])
    weight_one = gram_form(gram_table, r_map, change_map, False) / (
        gram_form(gram_table, change_map, change_map, False) + small_eps
    )
    step_mid = weight_one * lam_zero
    psi_mid_map = combine([(1.0, psi_map), (step_mid, {2: 1.0})])
    h_mid_map = combine([(1.0, ham_map), (step_mid, {3: 1.0})])
    r_mid_map = combine([(1.0, r_map), (-weight_one, change_map)])
    eps_mid = gram_form(gram_table, psi_mid_map, h_mid_map, False) / (
        gram_form(gram_table, psi_mid_map, psi_mid_map, False) + small_eps
    )
    level_mid = gram_form(gram_table, r_mid_map, r_mid_map, True) / (
        gram_form(gram_table, r_mid_map, r_mid_map, False) + small_eps
    )
    p_one = precondition(realize(r_mid_map, basis), kinetic, level_mid)
    g_one = apply_h(p_one)
    basis = [coeffs, h_zero, p_zero, g_zero, p_one, g_one]
    gram_table.update(gram_sums(basis, new_pairs(4, 6, (False,))))
    q_one_map = combine([(1.0, {5: 1.0}), (-eps_mid, {4: 1.0})])
    lam_one = -gram_form(gram_table, r_mid_map, q_one_map, False) / (
        gram_form(gram_table, q_one_map, q_one_map, False) + small_eps
    )
    new_map = combine([(1.0, psi_mid_map), (lam_one, {4: 1.0})])
    ham_new_map = combine([(1.0, h_mid_map), (lam_one, {5: 1.0})])
    norm_new = gram_form(gram_table, new_map, new_map, False) + small_eps
    energy = gram_form(gram_table, new_map, ham_new_map, False) / norm_new
    resid_map = combine([(1.0, ham_new_map), (-energy, new_map)])
    residual_norm = gram_form(gram_table, resid_map, resid_map, False) / norm_new
    new_bands = realize(new_map, basis)
    new_ham = realize(ham_new_map, basis)
    blank_rows = jnp.zeros((2, band_local, band_local * lax.axis_size("band")), jnp.float32)
    first_row = jnp.int32(0)
    over_rows = blank_rows
    ham_rows = blank_rows
    piece_bands = lax.all_gather(new_bands, "band", axis=1, tiled=True)
    piece_ham = lax.all_gather(new_ham, "band", axis=1, tiled=True)
    over_rows = lax.dynamic_update_slice_in_dim(
        over_rows, pair_products(new_bands, piece_bands), first_row, 2
    )
    ham_rows = lax.dynamic_update_slice_in_dim(
        ham_rows, pair_products(new_bands, piece_ham), first_row, 2
    )
    over_rows, ham_rows = (over_rows, ham_rows)
    over_rows, ham_rows = lax.psum((over_rows, ham_rows), "ga")
    correlation = over_rows / total_pw
    subspace = ham_rows / total_pw
    return (new_bands, energy, residual_norm, correlation, subspace)


QUAD = 4
TRIPLE = 3
MESH = pl.DeviceIdType.MESH


def split_const(values):
    high = np.asarray(values, np.float32).astype(jnp.bfloat16)
    low = (values - high.astype(np.float64)).astype(np.float32).astype(jnp.bfloat16)
    return np.stack([high, low])


def const_tables(grid_len, group):
    planes = grid_len // group
    chunks = planes // QUAD
    unit = 2.0 * np.pi / grid_len
    quarter = grid_len / 4.0
    chunk = np.arange(chunks)[:, None, None, None]
    dev = np.arange(group)[None, :, None, None]
    part = np.arange(2)[None, None, :, None]
    inner = np.arange(QUAD)[None, None, None, :]
    y_real = (dev * planes + chunk * QUAD + inner + 0 * part).reshape(-1)
    part_row = (part + 0 * (dev + chunk + inner)).reshape(-1)
    freq = np.arange(grid_len)
    phase = (y_real[:, None] * freq[None, :]) % grid_len
    tab_a = np.cos(unit * (phase - quarter * part_row[:, None]))
    tab_b = np.cos(unit * (phase + quarter * (1 - part_row[:, None])))
    wave = split_const(np.concatenate([tab_a, tab_b], axis=0))
    four = np.repeat(np.arange(4), grid_len)
    zed = np.tile(freq, 4)
    theta = 2.0 * np.pi * ((four[:, None] * four[None, :] % 4) / 4.0
                           + (zed[:, None] * zed[None, :] % grid_len) / grid_len)
    fourz = split_const(np.concatenate([np.cos(theta), np.sin(theta)], axis=1))
    dft = 2.0 * np.pi * np.outer(np.arange(group), np.arange(group)) / group
    real_mix = np.zeros((group, 2, QUAD, group, 2, QUAD))
    for row in range(QUAD):
        real_mix[:, 0, row, :, 0, row] = np.cos(dft)
        real_mix[:, 1, row, :, 1, row] = np.cos(dft)
        real_mix[:, 0, row, :, 1, row] = -np.sin(dft)
        real_mix[:, 1, row, :, 0, row] = np.sin(dft)
    size = group * 2 * QUAD
    real_mix = real_mix.reshape(size, size)

    def stacked(mat):
        high, low = split_const(mat)
        return np.concatenate([high, high, low], axis=1)

    across = np.stack([stacked(real_mix), stacked(real_mix.T)])
    b_lane = np.repeat(np.arange(TRIPLE), 4 * grid_len)
    a_lane = np.tile(np.repeat(np.arange(4), grid_len), TRIPLE)
    one = 2.0 * np.pi * (a_lane * b_lane) / planes
    two = unit * np.outer(np.arange(group), TRIPLE * a_lane + b_lane)
    lane_tw = np.stack([np.cos(one), np.sin(one)]).astype(np.float32)[:, None, :]
    dev_tw = np.stack([np.cos(two), np.sin(two)]).astype(np.float32)[:, :, None, :]
    return wave, fourz, across, lane_tw, dev_tw


def two_parts(values):
    high = values.astype(jnp.bfloat16)
    low = (values - high.astype(jnp.float32)).astype(jnp.bfloat16)
    return high, low


def bdot(left, right):
    return jnp.dot(left, right, preferred_element_type=jnp.float32)


def sweep_kernel(
    dims,
    coeffs_ref, cell_ref, potential_hbm, proj_hbm, strength_ref, atom_ref, chan_ref,
    wave_ref, fourz_hbm, across_ref, lane_ref, dev_ref,
    new_ref, scal_ref,
    hot_ref, hot_t_ref, ta_ref, tb_ref, key_ref, pot_ref, potential_ref, proj_ref, fourz_ref, in_sem,
    fsend, frecv, bsend, brecv, psend, precv, gsend, grecv, nsend, nrecv, isend, irecv, lsend, lrecv, csend, crecv,
    fs_sem, fr_sem, bs_sem, br_sem, ps_sem, pr_sem, gs_sem, gr_sem, ns_sem, nr_sem, cs_sem, cr_sem,
):
    group, bands, chunks, grid_len, total_pw, pw = dims
    rows = group * 2 * QUAD
    lanes = TRIPLE * 4 * grid_len
    quad_lanes = 4 * grid_len
    me = lax.axis_index("ga")
    band = lax.axis_index("band")

    loads = [
        pltpu.make_async_copy(source, target, in_sem.at[k])
        for k, (source, target) in enumerate(
            ((proj_hbm, proj_ref), (potential_hbm, potential_ref), (fourz_hbm, fourz_ref)))
    ]
    for load in loads:
        load.start()
    barrier = pltpu.get_barrier_semaphore()
    for off in range(1, group):
        pl.semaphore_signal(barrier, inc=1, device_id={"ga": lax.rem(me + off, group)}, device_id_type=MESH)
    for off in range(1, bands):
        pl.semaphore_signal(barrier, inc=1, device_id={"band": lax.rem(band + off, bands)}, device_id_type=MESH)

    def whole(values):
        return jnp.floor(values)

    cell = cell_ref[...].astype(jnp.float32)
    plane = whole((cell + 0.5) * (1.0 / (grid_len * grid_len)))
    in_plane = cell - plane * (grid_len * grid_len)
    y_num = whole((in_plane + 0.5) * (1.0 / grid_len))
    z_num = in_plane - y_num * grid_len
    key_ref[...] = plane * grid_len + z_num

    def signed(values):
        return jnp.where(2.0 * values < grid_len, values, values - grid_len)

    f_x = signed(plane * group + me.astype(jnp.float32))
    f_y, f_z = signed(y_num), signed(z_num)
    kin = kin_unit * (f_x * f_x + f_y * f_y + f_z * f_z)

    def build_hot(step, carry):
        at = pl.multiple_of(step * 128, 128)
        key_col = jnp.transpose(jnp.broadcast_to(key_ref[:, pl.ds(at, 128)], (128, 128)))
        lane_id = lax.broadcasted_iota(jnp.int32, (128, 128), 1).astype(jnp.float32)
        for k in range(lanes // 128):
            hit = jnp.where(lane_id == key_col - 128.0 * k, 1.0, 0.0)
            hot_ref[pl.ds(at, 128), k * 128:(k + 1) * 128] = hit.astype(jnp.bfloat16)
        return carry

    lax.fori_loop(0, pw // 128, build_hot, 0)
    y_hot = jnp.where(lax.broadcasted_iota(jnp.int32, (grid_len, pw), 0).astype(jnp.float32) == y_num, 1.0, 0.0).astype(jnp.bfloat16)
    for part in range(chunks):
        for table, base in ((ta_ref, 0), (tb_ref, chunks * rows)):
            at = base + part * rows
            table[part] = bdot(wave_ref[0, at:at + rows, :], y_hot) + bdot(wave_ref[1, at:at + rows, :], y_hot)

    def build_turn():
        turn_rows = 128

        def step_turn(step, carry):
            at = pl.multiple_of(step * turn_rows, turn_rows)
            row_id = (lax.broadcasted_iota(jnp.int32, (turn_rows, pw), 0) + at).astype(jnp.float32)
            hot_t_ref[pl.ds(at, turn_rows), :] = jnp.where(row_id == key_ref[...], 1.0, 0.0).astype(jnp.bfloat16)
            return carry

        lax.fori_loop(0, lanes // turn_rows, step_turn, 0)

    def build_potential():
        for part in range(chunks):
            for b in range(TRIPLE):
                for a in range(4):
                    at = (b * 4 + a) * grid_len
                    block = potential_ref[:, TRIPLE * a + b, part * QUAD:(part + 1) * QUAD, :] * (1.0 / grid_len**3)
                    pot_ref[part, :, :QUAD, at:at + grid_len] = block
                    pot_ref[part, :, QUAD:, at:at + grid_len] = block

    def build_coupling():
        atoms, chans = strength_ref.shape[0] // strength_ref.shape[1], strength_ref.shape[1]
        size = atoms * chans
        ident = atom_ref[...] * chans + chan_ref[...]
        hot = (lax.broadcasted_iota(jnp.int32, (size, ident.shape[1]), 0) == ident).astype(jnp.float32)
        row_at = lax.broadcasted_iota(jnp.int32, (size, size), 0)
        col_at = lax.broadcasted_iota(jnp.int32, (size, size), 1)
        tiled = jnp.concatenate([strength_ref[...]] * atoms, axis=1)
        same = (row_at // chans == col_at // chans).astype(jnp.float32)
        block = tiled * same
        block = 0.5 * (block + jnp.transpose(block))
        half = lax.dot_general(hot, block, (((0,), (0,)), ((), ())), precision=top_precision, preferred_element_type=jnp.float32)
        return jnp.dot(half, hot, precision=top_precision, preferred_element_type=jnp.float32)

    pl.semaphore_wait(barrier, group + bands - 2)

    sign = jnp.where(lax.broadcasted_iota(jnp.int32, (1, 2 * QUAD, 1), 1) < QUAD, -1.0, 1.0).astype(jnp.float32)

    def times_i(values):
        return pltpu.roll(values, QUAD, 1) * sign

    def lane_split(values):
        return [values[..., k * quad_lanes:(k + 1) * quad_lanes] for k in range(TRIPLE)]

    def mix_fourz(triple, direction):
        stacked = jnp.concatenate([t.reshape(rows, quad_lanes) for t in triple], axis=0)
        high, low = two_parts(stacked)
        out = bdot(high, fourz_ref[0]) + bdot(low, fourz_ref[0]) + bdot(high, fourz_ref[1])
        out = out.reshape(TRIPLE * group, 2 * QUAD, 2 * quad_lanes)
        mixed = out[..., :quad_lanes] + direction * times_i(out[..., quad_lanes:])
        return [mixed[k * group:(k + 1) * group] for k in range(TRIPLE)]

    def turn_lane(triple, direction):
        done = [triple[0]]
        for k in range(1, TRIPLE):
            at = slice(k * quad_lanes, (k + 1) * quad_lanes)
            done.append(triple[k] * lane_ref[0, :, at][None] + direction * times_i(triple[k]) * lane_ref[1, :, at][None])
        return done

    def three(triple, direction):
        total = triple[1] + triple[2]
        diff = times_i(triple[1] - triple[2]) * (direction * 0.8660254037844386)
        base = triple[0] - 0.5 * total
        return [triple[0] + total, base + diff, base - diff]

    def turn_dev(values, direction):
        return values * dev_ref[0] + direction * times_i(values) * dev_ref[1]

    def mix_devices(values, which):
        high, low = two_parts(values.reshape(rows, lanes))
        return bdot(across_ref[which], jnp.concatenate([high, low, high], axis=0))

    def all_sum(local, send, recv, send_sem, recv_sem, shape_at):
        send[shape_at] = local
        recv[shape_at, me] = local
        for off in range(1, group):
            pltpu.make_async_remote_copy(
                src_ref=send.at[shape_at], dst_ref=recv.at[shape_at, me],
                send_sem=send_sem.at[shape_at, off - 1], recv_sem=recv_sem.at[shape_at, off - 1],
                device_id={"ga": lax.rem(me + off, group)}, device_id_type=MESH).start()

    def all_sum_end(send, recv, send_sem, recv_sem, shape_at):
        for off in range(1, group):
            pltpu.make_async_remote_copy(
                src_ref=send.at[shape_at], dst_ref=recv.at[shape_at, lax.rem(me + group - off, group)],
                send_sem=send_sem.at[shape_at, off - 1], recv_sem=recv_sem.at[shape_at, off - 1],
                device_id={"ga": lax.rem(me + off, group)}, device_id_type=MESH).wait()
        running = recv[shape_at, 0]
        for dev in range(1, group):
            running = running + recv[shape_at, dev]
        return running

    def piece(turn, part, off, send, recv, send_sem, recv_sem, incoming):
        peer = lax.rem(me + off, group)
        source = lax.rem(me + group - off, group) if incoming else me
        return pltpu.make_async_remote_copy(
            src_ref=send.at[turn, part, peer], dst_ref=recv.at[turn, part, source],
            send_sem=send_sem.at[turn, part, off - 1], recv_sem=recv_sem.at[turn, part, off - 1],
            device_id={"ga": peer}, device_id_type=MESH)

    def apply_h(turn, vector):
        v_re, v_im = vector[0:1], vector[1:2]
        fwd = (fsend, frecv, fs_sem, fr_sem)
        back = (bsend, brecv, bs_sem, br_sem)

        def put(part, carry):
            high, low = two_parts(ta_ref[part] * v_re + tb_ref[part] * v_im)
            out = bdot(jnp.concatenate([high, low], axis=0), hot_ref[...])
            out = (out[:rows] + out[rows:]).reshape(group, 2 * QUAD, lanes)
            fsend[turn, part] = out
            frecv[turn, part, me] = fsend[turn, part, me]
            for off in range(1, group):
                piece(turn, part, off, *fwd, False).start()
            return carry

        lax.fori_loop(0, chunks, put, 0)
        if turn == 0:
            for load in loads:
                load.wait()
        sums = lax.dot_general(vector, proj_ref[...], (((1,), (1,)), ((), ())), precision=top_precision, preferred_element_type=jnp.float32)
        all_sum(sums, psend, precv, ps_sem, pr_sem, turn)
        if turn == 0:
            build_potential()
            shared.append(build_coupling())
            build_turn()

        def middle(part, carry):
            for off in range(1, group):
                piece(turn, part, off, *fwd, True).wait()
            triple = turn_lane(three(lane_split(frecv[turn, part]), 1.0), 1.0)
            values = turn_dev(jnp.concatenate(mix_fourz(triple, 1.0), axis=-1), 1.0)
            values = mix_devices(values, 0) * pot_ref[part].reshape(rows, lanes)
            values = mix_devices(values, 1).reshape(group, 2 * QUAD, lanes)
            triple = mix_fourz(lane_split(turn_dev(values, -1.0)), -1.0)
            triple = three(turn_lane(triple, -1.0), -1.0)
            bsend[turn, part] = jnp.concatenate(triple, axis=-1)
            brecv[turn, part, me] = bsend[turn, part, me]
            for off in range(1, group):
                piece(turn, part, off, *back, False).start()
            return carry

        lax.fori_loop(0, chunks, middle, 0)
        sums = all_sum_end(psend, precv, ps_sem, pr_sem, turn) * (1.0 / total_pw)
        half = sums.shape[1] // 2
        pair = jnp.concatenate([
            sums[0:1, :half] + sums[1:2, half:], sums[1:2, :half] - sums[0:1, half:]], axis=0)
        mixed = jnp.dot(pair, shared[0], precision=top_precision, preferred_element_type=jnp.float32)
        m_re, m_im = mixed[0:1], mixed[1:2]
        weights = jnp.concatenate([
            jnp.concatenate([m_re, -m_im], axis=1), jnp.concatenate([m_im, m_re], axis=1)], axis=0)
        nonlocal_part = jnp.dot(weights, proj_ref[...], precision=top_precision, preferred_element_type=jnp.float32)
        start = kin * vector + nonlocal_part

        def take(part, carry):
            run_re, run_im = carry
            for off in range(1, group):
                piece(turn, part, off, *back, True).wait()
            high, low = two_parts(brecv[turn, part].reshape(rows, lanes))
            out = bdot(jnp.concatenate([high, low], axis=0), hot_t_ref[...])
            out = out[:rows] + out[rows:]
            run_re = run_re + jnp.sum(ta_ref[part] * out, axis=0, keepdims=True)
            run_im = run_im + jnp.sum(tb_ref[part] * out, axis=0, keepdims=True)
            return run_re, run_im

        run_re, run_im = lax.fori_loop(0, chunks, take, (start[0:1], start[1:2]))
        return jnp.concatenate([run_re, run_im], axis=0)

    def as_row(values):
        total = jnp.sum(jnp.sum(values, axis=0, keepdims=True), axis=1, keepdims=True)
        return jnp.broadcast_to(total, (1, 128))

    row_count = gsend.shape[1]

    def gram_sums(turn, basis, pair_list):
        found_rows = []
        for one, two, use_kin in pair_list:
            product = basis[one] * basis[two]
            found_rows.append(as_row(product * kin if use_kin else product))
        found_rows += [jnp.zeros((1, 128), jnp.float32)] * (row_count - len(found_rows))
        all_sum(jnp.concatenate(found_rows, axis=0), gsend, grecv, gs_sem, gr_sem, turn)
        summed = all_sum_end(gsend, grecv, gs_sem, gr_sem, turn) * (1.0 / total_pw)
        found = {}
        for slot, (one, two, use_kin) in enumerate(pair_list):
            value = summed[slot:slot + 1]
            found[use_kin, one, two] = value
            found[use_kin, two, one] = value
        return found

    def realize(coef_map, basis):
        running = 0.0
        for index, coef in coef_map.items():
            running = running + (basis[index] if isinstance(coef, float) and coef == 1.0 else spread_row(coef) * basis[index])
        return running

    def spread_row(coef):
        return coef if isinstance(coef, float) else coef[:, 0:1]

    def smooth(residual, level):
        ratio = kin / (1.5 * level[:, 0:1] + 1.0)
        poly = 27.0 + ratio * (18.0 + ratio * (12.0 + 8.0 * ratio))
        square = ratio * ratio
        return residual * (poly / (poly + 16.0 * square * square))

    shared = []
    coeffs = coeffs_ref[:, 0, :]
    h_zero = apply_h(0, coeffs)
    basis = [coeffs, h_zero]
    gram = gram_sums(0, basis, new_pairs(0, 2, (False, True)))
    psi = {0: 1.0}
    ham = {1: 1.0}
    eps_zero = gram_form(gram, psi, ham, False) / (gram_form(gram, psi, psi, False) + small_eps)
    r_map = combine([(1.0, ham), (-eps_zero, psi)])
    level = gram_form(gram, r_map, r_map, True) / (gram_form(gram, r_map, r_map, False) + small_eps)
    p_zero = smooth(realize(r_map, basis), level)
    g_zero = apply_h(1, p_zero)
    basis += [p_zero, g_zero]
    gram.update(gram_sums(1, basis, new_pairs(2, 4, (False, True))))
    q_map = combine([(1.0, {3: 1.0}), (-eps_zero, {2: 1.0})])
    lam_zero = -gram_form(gram, r_map, q_map, False) / (gram_form(gram, q_map, q_map, False) + small_eps)
    psi_one = combine([(1.0, psi), (lam_zero, {2: 1.0})])
    h_one = combine([(1.0, ham), (lam_zero, {3: 1.0})])
    eps_one = gram_form(gram, psi_one, h_one, False) / (gram_form(gram, psi_one, psi_one, False) + small_eps)
    r_one = combine([(1.0, h_one), (-eps_one, psi_one)])
    change = combine([(1.0, r_map), (-1.0, r_one)])
    weight = gram_form(gram, r_map, change, False) / (gram_form(gram, change, change, False) + small_eps)
    step = weight * lam_zero
    psi_mid = combine([(1.0, psi), (step, {2: 1.0})])
    h_mid = combine([(1.0, ham), (step, {3: 1.0})])
    r_mid = combine([(1.0, r_map), (-weight, change)])
    eps_mid = gram_form(gram, psi_mid, h_mid, False) / (gram_form(gram, psi_mid, psi_mid, False) + small_eps)
    level = gram_form(gram, r_mid, r_mid, True) / (gram_form(gram, r_mid, r_mid, False) + small_eps)
    p_one = smooth(realize(r_mid, basis), level)

    def swap(which, send, recv, off, incoming):
        source = lax.rem(band + bands - off, bands) if incoming else band
        return pltpu.make_async_remote_copy(
            src_ref=send, dst_ref=recv.at[source],
            send_sem=ns_sem.at[which, off - 1], recv_sem=nr_sem.at[which, off - 1],
            device_id={"band": lax.rem(band + off, bands)}, device_id_type=MESH)

    def share(which, send, recv, values):
        send[...] = values
        recv[band] = values
        for off in range(1, bands):
            swap(which, send, recv, off, False).start()

    share(0, nsend, nrecv, jnp.stack([realize(psi_mid, basis), p_one, realize(h_mid, basis)]))
    g_one = apply_h(2, p_one)
    share(1, isend, irecv, g_one)
    basis += [p_one, g_one]
    gram.update(gram_sums(2, basis, new_pairs(4, 6, (False,))))
    q_one = combine([(1.0, {5: 1.0}), (-eps_mid, {4: 1.0})])
    lam_one = -gram_form(gram, r_mid, q_one, False) / (gram_form(gram, q_one, q_one, False) + small_eps)
    new_map = combine([(1.0, psi_mid), (lam_one, {4: 1.0})])
    ham_new = combine([(1.0, h_mid), (lam_one, {5: 1.0})])
    norm_new = gram_form(gram, new_map, new_map, False) + small_eps
    energy = gram_form(gram, new_map, ham_new, False) / norm_new
    resid = combine([(1.0, ham_new), (-energy, new_map)])
    resid_norm = gram_form(gram, resid, resid, False) / norm_new
    new = realize(new_map, basis)
    new_h = realize(ham_new, basis)
    new_ref[...] = new
    share(2, lsend, lrecv, jnp.broadcast_to(lam_one, (8, 128)))
    for which, send, recv in ((0, nsend, nrecv), (1, isend, irecv), (2, lsend, lrecv)):
        for off in range(1, bands):
            swap(which, send, recv, off, True).wait()
    found_rows = []
    others = []
    for other in range(bands):
        lam = lrecv[other, 0:1, 0:1]
        others.append((nrecv[other, 0] + lam * nrecv[other, 1], nrecv[other, 2] + lam * irecv[other]))
    for first in (0, 1):
        for imag in (False, True):
            for other in range(bands):
                o_re = others[other][first][0:1]
                o_im = others[other][first][1:2]
                if imag:
                    found_rows.append(as_row(new[0:1] * o_im - new[1:2] * o_re))
                else:
                    found_rows.append(as_row(new[0:1] * o_re + new[1:2] * o_im))
    all_sum(jnp.concatenate(found_rows, axis=0), csend, crecv, cs_sem, cr_sem, 0)
    summed = all_sum_end(csend, crecv, cs_sem, cr_sem, 0) * (1.0 / total_pw)
    scal_ref[...] = jnp.concatenate([summed, energy, resid_norm, jnp.zeros((6, 128), jnp.float32)], axis=0)


def finish_kernel(bands, new_ref, scal_ref, bands_ref, energy_ref, norm_ref, corr_ref, sub_ref):
    bands_ref[:, 0, :] = new_ref[...]
    lane = lax.broadcasted_iota(jnp.int32, (1, bands), 1)
    for ref, base in ((corr_ref, 0), (sub_ref, 2 * bands)):
        for part in range(2):
            row = jnp.zeros((1, bands), jnp.float32)
            for other in range(bands):
                at = base + part * bands + other
                row = jnp.where(lane == other, scal_ref[at:at + 1, :bands], row)
            ref[part] = row
    energy_ref[0] = scal_ref[4 * bands, 0]
    norm_ref[0] = scal_ref[4 * bands + 1, 0]


def kernel_body(coeffs, cell_map, potential, projectors, strengths, proj_atom, proj_chan):
    group = lax.axis_size("ga")
    bands = lax.axis_size("band")
    grid_len = potential.shape[0]
    planes = grid_len // group
    chunks = planes // QUAD
    pw = coeffs.shape[2]
    total_pw = pw * group
    rows = group * 2 * QUAD
    lanes = planes * grid_len
    proj_rows = 2 * projectors.shape[1]
    tables = [jnp.asarray(t) for t in const_tables(grid_len, group)]
    gram_rows = 16
    piece_shape = (3, chunks, group, 2 * QUAD, lanes)
    dma = pltpu.SemaphoreType.DMA
    vmem = pl.BlockSpec(memory_space=pltpu.VMEM)
    far = pl.BlockSpec(memory_space=pl.ANY)
    f32 = jnp.float32
    new, scal = pl.pallas_call(
        functools.partial(sweep_kernel, (group, bands, chunks, grid_len, total_pw, pw)),
        out_shape=(
            jax.ShapeDtypeStruct((2, pw), f32),
            jax.ShapeDtypeStruct((4 * bands + 8, 128), f32),
        ),
        in_specs=[vmem, vmem, far, far] + [vmem] * 4 + [far] + [vmem] * 3,
        out_specs=(vmem, vmem),
        scratch_shapes=[
            pltpu.VMEM((pw, lanes), jnp.bfloat16),
            pltpu.VMEM((lanes, pw), jnp.bfloat16),
            pltpu.VMEM((chunks, rows, pw), f32),
            pltpu.VMEM((chunks, rows, pw), f32),
            pltpu.VMEM((1, pw), f32),
            pltpu.VMEM((chunks, group, 2 * QUAD, lanes), f32),
            pltpu.VMEM((group, planes, planes, grid_len), f32),
            pltpu.VMEM((proj_rows, pw), f32),
            pltpu.VMEM(tables[1].shape, jnp.bfloat16),
            pltpu.SemaphoreType.DMA((3,)),
            pltpu.VMEM(piece_shape, f32),
            pltpu.VMEM(piece_shape, f32),
            pltpu.VMEM(piece_shape, f32),
            pltpu.VMEM(piece_shape, f32),
            pltpu.VMEM((3, 2, proj_rows), f32),
            pltpu.VMEM((3, group, 2, proj_rows), f32),
            pltpu.VMEM((3, gram_rows, 128), f32),
            pltpu.VMEM((3, group, gram_rows, 128), f32),
            pltpu.VMEM((3, 2, pw), f32),
            pltpu.VMEM((bands, 3, 2, pw), f32),
            pltpu.VMEM((2, pw), f32),
            pltpu.VMEM((bands, 2, pw), f32),
            pltpu.VMEM((8, 128), f32),
            pltpu.VMEM((bands, 8, 128), f32),
            pltpu.VMEM((1, 4 * bands, 128), f32),
            pltpu.VMEM((1, group, 4 * bands, 128), f32),
            dma((3, chunks, group - 1)), dma((3, chunks, group - 1)),
            dma((3, chunks, group - 1)), dma((3, chunks, group - 1)),
            dma((3, group - 1)), dma((3, group - 1)),
            dma((3, group - 1)), dma((3, group - 1)),
            dma((3, bands - 1)), dma((3, bands - 1)),
            dma((1, group - 1)), dma((1, group - 1)),
        ],
        compiler_params=pltpu.CompilerParams(
            collective_id=0, has_side_effects=True, vmem_limit_bytes=60 * 1024 * 1024
        ),
        name="sweeps",
    )(
        coeffs, cell_map.reshape(1, pw), potential.reshape(group, planes, planes, grid_len),
        projectors.reshape(proj_rows, pw), strengths.reshape(-1, strengths.shape[2]),
        proj_atom.reshape(1, -1), proj_chan.reshape(1, -1), *tables,
    )

    smem = pl.BlockSpec(memory_space=pltpu.SMEM)
    return pl.pallas_call(
        functools.partial(finish_kernel, bands),
        out_shape=(
            jax.ShapeDtypeStruct((2, 1, pw), f32),
            jax.ShapeDtypeStruct((1,), f32),
            jax.ShapeDtypeStruct((1,), f32),
            jax.ShapeDtypeStruct((2, 1, bands), f32),
            jax.ShapeDtypeStruct((2, 1, bands), f32),
        ),
        in_specs=[vmem, vmem],
        out_specs=(vmem, smem, smem, vmem, vmem),
        name="finish",
    )(new, scal)


def body(coeffs, cell_map, potential, projectors, strengths, proj_atom, proj_chan):
    group = lax.axis_size("ga")
    grid_len = potential.shape[0]
    planes = grid_len // group
    fits = (
        planes == 4 * TRIPLE
        and 4 * grid_len % 128 == 0
        and coeffs.shape[1] == 1
        and coeffs.shape[2] % 256 == 0
        and 2 * projectors.shape[1] == 128
    )
    chosen = kernel_body if fits else plain_body
    return chosen(coeffs, cell_map, potential, projectors, strengths, proj_atom, proj_chan)


def solution(mesh):
    placed = (
        P(None, "band", "ga"),
        P("ga"),
        P(None, "ga", None),
        P(None, None, "ga"),
        P(),
        P(),
        P(),
    )
    return jax.shard_map(
        body,
        mesh=mesh,
        in_specs=placed,
        out_specs=(
            P(None, "band", "ga"),
            P("band"),
            P("band"),
            P(None, "band", None),
            P(None, "band", None),
        ),
        check_vma=False,
    )
```
